32 devices in a mesh: dp: 16 (over z, y, core), mp: 2 (over x).
Axes of the slice: x: 2, y: 2, z: 4, core: 2. Of those that a mesh axis runs over, the one named last changes fastest.
Arguments:
- hidden: bfloat16 [512, 7168], P('dp', 'mp'), may hold values from -12 to 12
- steering: float32 [7168], P('mp'), may hold values from -3 to 3
- norm_gain: bfloat16 [7168], P('mp'), may hold values from 0.099609375 to 1.8984375
- target: bfloat16 [512, 7168], P('dp', 'mp'), may hold values from -8 to 8
- routes: int32 [512, 8], P('dp'), may hold values from 0 to 15, all different within a row; in each aligned block of 32 rows (0 to 31, 32 to 63, ...) at most 20 rows name the same one
- gate_probs: float32 [512, 8], P('dp'), may hold values from 0.05 to 0.3
- contrast: int32 [512], P('dp'), may hold values from 0 to 1
- gate_weight: bfloat16 [16, 7168, 2048], P('dp', None, 'mp'), may hold values from -0.0625 to 0.0625
- up_weight: bfloat16 [16, 7168, 2048], P('dp', None, 'mp'), may hold values from -0.0625 to 0.0625
- down_weight: bfloat16 [16, 2048, 7168], P('dp', 'mp'), may hold values from -0.125 to 0.125
Outputs:
- mixed: bfloat16 [512, 7168], P('dp', 'mp')
- steer_grad: float32 [7168], P('mp')
The draws below stay inside these ranges and needn't reach their ends.
Inputs may be any that keep to these rules, and one draw needn't show every extreme that they name: `routes`: each row names 8 different experts; among the 32 rows of one index of dp no expert is named by more than 20 rows.
All inputs are finite; a program needn't handle non-finite values.
Results may differ from the reference program's by a relative error of at most 0.005.
Values may be sent and summed in bfloat16 or wider, within the bound.
No kernel may reach another device: no remote copies, remote signals or barrier semaphores. Data moves between devices by JAX's collectives and lax.ppermute only.
A program may use at most 128 MiB of HBM per device.

```python
import math
import jax
import jax.numpy as jnp
import numpy as np
from jax import lax

D = 7168
FF = 2048
TOP = 8
TOK_DEV = 32
EXPERTS = 16
TOKENS = 512
CAP = 20
N_DP = 16
N_MP = 2


def draw_hidden(key, part):
    key_list = jax.random.split(jax.random.fold_in(key, 11), 3)
    row_scale = jnp.exp(jax.random.uniform(key_list[0], (TOKENS, 1), jnp.float32, math.log(0.3), math.log(3.0)))
    col_scale = jnp.exp(math.log(3.0) * jnp.arange(D, dtype=jnp.float32)[None, :] / D + jax.random.uniform(key_list[1], (1, D), jnp.float32, math.log(0.6), math.log(1.6)))
    base_draw = jax.random.normal(key_list[2], (TOKENS, D), jnp.float32)
    return jnp.clip(0.5 * base_draw * row_scale * col_scale, -12.0, 12.0).astype(jnp.bfloat16)


def draw_target(key, part):
    key_list = jax.random.split(jax.random.fold_in(key, 23), 2)
    row_scale = jnp.exp(math.log(3.0) * jnp.arange(TOKENS, dtype=jnp.float32)[:, None] / TOKENS + jax.random.uniform(key_list[0], (TOKENS, 1), jnp.float32, math.log(0.5), math.log(2.0)))
    base_draw = jax.random.normal(key_list[1], (TOKENS, D), jnp.float32)
    return jnp.clip(0.6 * base_draw * row_scale, -8.0, 8.0).astype(jnp.bfloat16)


def touch_ends(array, rng, least, top_value):
    index_at = [jax.random.randint(jax.random.fold_in(rng, axis), (), 0, length) for axis, length in enumerate(array.shape)]
    widest = array.shape.index(max(array.shape))
    beside = index_at[:widest] + [(index_at[widest] + 1) % array.shape[widest]] + index_at[widest + 1:]
    return array.at[tuple(index_at)].set(least).at[tuple(beside)].set(top_value)


def levels(own_key, extent, cuts, least, high):
    factor_of, own = 1.0, jax.random.fold_in(own_key, 6)
    for dim, shards_of in cuts:
        heights = jnp.exp(jax.random.uniform(jax.random.fold_in(own, dim), (shards_of,), jnp.float32, least / len(cuts), high / len(cuts)))
        factor_of = factor_of * jnp.repeat(heights, extent[dim] // shards_of).reshape([-1 if axis == dim else 1 for axis in range(len(extent))])
    return factor_of


def assign_block(rng, own, number, rows, number_of, top, most, slope):
    sequence = jax.random.permutation(rng, number_of)
    packed, common = shares(number_of, rows * top, most, slope, True), shares(number_of, rows * top, most, slope, False)
    places = jnp.arange(number_of)

    def named(lengths, turn):
        used = int((lengths > 0).sum())
        fixed = max(1, used // 4)
        moved = fixed + (places - fixed + turn * (used - fixed)) % max(1, number_of - fixed)
        return jnp.zeros((number_of,), jnp.int32).at[sequence[jnp.where(places < fixed, places, moved)]].set(jnp.asarray(lengths, jnp.int32))

    lengths = jnp.where(number % 4 == 0, named(packed, number // 4), named(common, number - number // 4 - 1))
    mixed = jax.random.permutation(jax.random.fold_in(own, 3), number_of)
    donor, taker = mixed[0:number_of // 2 * 2:2], mixed[1:number_of // 2 * 2:2]
    room = jnp.minimum(lengths[donor] - 1, most - lengths[taker]) // 2
    room = jnp.where((donor == sequence[0]) | (taker == sequence[0]) | (lengths[taker] == 0), 0, jnp.maximum(room, 0))
    moved = jax.random.randint(jax.random.fold_in(own, 4), (number_of // 2,), 0, 1 << 20) % (room + 1)
    lengths = lengths.at[donor].add(-moved).at[taker].add(moved)
    members = jnp.searchsorted(jnp.cumsum(lengths), jnp.arange(rows * top), side="right").astype(jnp.int32)
    listing = members.reshape(top, rows).T
    listing = listing[jax.random.permutation(jax.random.fold_in(own, 1), rows)]
    turn = jax.random.randint(jax.random.fold_in(own, 2), (rows, 1), 0, top)
    return jnp.take_along_axis(listing, (jnp.arange(top)[None, :] + turn) % top, axis=1)


def shares(count, total, most, skew, full):
    loads = [(1 << 20) // math.isqrt(grade ** skew) + 1 for grade in range(1, count + 1)]
    largest = most if full else min(most, max(-(-total // count), total * loads[0] // sum(loads)))
    least = 1 if total - largest >= count - 1 else 0
    holding, spare = [largest] + [least] * (count - 1), total - largest - least * (count - 1)
    while spare > 0:
        candidates = [i for i in range(1, count) if holding[i] < largest] or [i for i in range(1, count) if holding[i] < most]
        pool, remaining = sum([loads[i] for i in candidates]), spare
        for i in candidates:
            more = min(most - holding[i], max(1, remaining * loads[i] // pool), spare)
            holding[i] = holding[i] + more
            spare = spare - more
    return np.array(holding)


def normal_values(own_key, dims, scale, most, cuts=(), held_as=jnp.bfloat16):
    values = jax.random.normal(own_key, dims, jnp.float32) * scale
    if len(cuts) > 0:
        values = levels(own_key, dims, cuts, -0.22, 0.18) * values
    return jnp.clip(values, min=-most, max=most).astype(held_as)


def setup_inputs(seed: int = 0) -> dict:
    arg_keys = jax.random.split(jax.random.key(seed), 11)
    hidden = draw_hidden(jax.random.fold_in(arg_keys[10], 71), 0)
    steering = normal_values(arg_keys[1], (D,), 0.5, 3.0, ((0, 2),), jnp.float32)
    norm_gain = jnp.clip(1.0 + 0.18 * jax.random.normal(arg_keys[2], (D,), jnp.float32), 0.099609375, 1.8984375).astype(jnp.bfloat16)
    target = draw_target(jax.random.fold_in(arg_keys[10], 71), 0)
    routes_keys = jax.random.split(jax.random.fold_in(arg_keys[4], 1), TOKENS // TOK_DEV)
    routes_turns = jax.random.permutation(jax.random.fold_in(arg_keys[4], 3), TOKENS // TOK_DEV)
    routes = jax.vmap(lambda own, number: assign_block(jax.random.fold_in(arg_keys[4], 2), own, number, TOK_DEV, EXPERTS, TOP, CAP, 1))(routes_keys, routes_turns).reshape((TOKENS, TOP))
    gate_probs = jnp.clip(0.05 + 0.25 * jax.random.uniform(arg_keys[5], (TOKENS, TOP), jnp.float32) ** levels(arg_keys[5], (TOKENS, TOP), ((0, 16),), -0.2, 0.2), 0.05, 0.3)
    contrast = touch_ends(jax.random.randint(arg_keys[6], (TOKENS,), 0, 2), jax.random.fold_in(arg_keys[6], 1), 0, 1).astype(jnp.int32)
    gate_weight = normal_values(arg_keys[7], (EXPERTS, D, FF), D ** -0.5, 0.0625, ((0, 16), (2, 2)))
    up_weight = normal_values(arg_keys[8], (EXPERTS, D, FF), D ** -0.5, 0.0625, ((0, 16), (2, 2)))
    down_weight = normal_values(arg_keys[9], (EXPERTS, FF, D), FF ** -0.5, 0.125, ((0, 16), (1, 2)))
    return {"hidden": hidden, "steering": steering, "norm_gain": norm_gain, "target": target, "routes": routes, "gate_probs": gate_probs, "contrast": contrast, "gate_weight": gate_weight, "up_weight": up_weight, "down_weight": down_weight}


EPSILON = 1e-06

def reference(hidden, steering, norm_gain, target, routes, gate_probs, contrast, gate_weight, up_weight, down_weight):
    stream = hidden.astype(jnp.float32) + steering.astype(jnp.float32)[None, :]
    inverse = lax.rsqrt(lax.optimization_barrier(jnp.mean(stream * stream, axis=1, keepdims=True)) + EPSILON)
    gain_row = norm_gain.astype(jnp.float32)[None, :]
    normed = (stream * inverse * gain_row).astype(jnp.bfloat16)
    sign_col = (2 * contrast - 1).astype(jnp.float32)[:, None]
    cotangent = target.astype(jnp.float32) * sign_col
    capacity_rows = N_DP * CAP
    quarter_size = FF // N_MP

    def one_expert(state_pair, inputs):
        out_total, grad_total = state_pair
        gate_mat, up_mat, down_mat, expert = inputs
        chosen = routes == expert
        weight_tok = lax.optimization_barrier(jnp.sum(jnp.where(chosen, gate_probs, jnp.zeros((), gate_probs.dtype)), axis=1))
        picked = jnp.any(chosen, axis=1).astype(jnp.int32)
        row_order = jnp.argsort(-picked, stable=True)[:capacity_rows].astype(jnp.int32)
        is_valid = picked[row_order] == 1
        rows_in = jnp.where(is_valid[:, None], normed[row_order], jnp.zeros((), jnp.bfloat16))
        weight_rows = weight_tok[row_order]
        grad_rows = (weight_rows[:, None] * cotangent[row_order]).astype(jnp.bfloat16)
        gate_pre = jnp.dot(rows_in, gate_mat, preferred_element_type=jnp.float32)
        up_pre = jnp.dot(rows_in, up_mat, preferred_element_type=jnp.float32)
        back_hidden = jnp.dot(grad_rows, down_mat.T, preferred_element_type=jnp.float32)
        sigma_gate = jax.nn.sigmoid(gate_pre)
        activated = (gate_pre * sigma_gate * up_pre).astype(jnp.bfloat16)
        grad_gate = (back_hidden * up_pre * sigma_gate * (1.0 + gate_pre * (1.0 - sigma_gate))).astype(jnp.bfloat16)
        grad_up = (back_hidden * gate_pre * sigma_gate).astype(jnp.bfloat16)
        out_rows = jnp.zeros((capacity_rows, D), jnp.float32)
        grad_back = jnp.zeros((capacity_rows, D), jnp.float32)
        for quarter_index in range(N_MP):
            low = quarter_index * quarter_size
            high = low + quarter_size
            out_part = jnp.dot(activated[:, low:high], down_mat[low:high], preferred_element_type=jnp.float32).astype(jnp.bfloat16)
            grad_part = (jnp.dot(grad_gate[:, low:high], gate_mat[:, low:high].T, preferred_element_type=jnp.float32) + jnp.dot(grad_up[:, low:high], up_mat[:, low:high].T, preferred_element_type=jnp.float32)).astype(jnp.bfloat16)
            out_rows = out_rows + lax.optimization_barrier(out_part).astype(jnp.float32)
            grad_back = grad_back + lax.optimization_barrier(grad_part).astype(jnp.float32)
        out_total = out_total.at[row_order].add(weight_rows[:, None] * out_rows)
        grad_total = grad_total.at[row_order].add(grad_back)
        return ((out_total, grad_total), None)
    start_pair = (jnp.zeros((TOKENS, D), jnp.float32), jnp.zeros((TOKENS, D), jnp.float32))
    expert_ids = jnp.arange(EXPERTS, dtype=jnp.int32)
    (out_sum, grad_sum), unused = lax.scan(one_expert, start_pair, (gate_weight, up_weight, down_weight, expert_ids))
    mixed = (stream + out_sum).astype(jnp.bfloat16)
    project = lax.optimization_barrier(jnp.sum(stream * gain_row * grad_sum, axis=1, keepdims=True))
    grad_stream = cotangent + inverse * gain_row * grad_sum - stream * inverse * inverse * inverse * project / D
    steer_grad = lax.optimization_barrier(jnp.sum(grad_stream, axis=0))
    return (mixed, steer_grad)
```

```python
import jax
import jax.numpy as jnp
from jax import lax
from jax.sharding import PartitionSpec as P

EPSILON = 1e-06
BF16 = jnp.bfloat16
F32 = jnp.float32
BOTH = ("dp", "mp")


def thirds(values):
    high = lax.reduce_precision(values, 8, 7)
    rest = values - high
    middle = lax.reduce_precision(rest, 8, 7)
    low = rest - middle
    return high.astype(BF16), middle.astype(BF16), low.astype(BF16)


def rows_times(values, matrix, contracted):
    rows = jnp.stack(thirds(values))
    return jnp.sum(
        lax.dot_general(rows, matrix, (((1,), (contracted,)), ((), ())), preferred_element_type=F32),
        axis=0,
    )


def forward(normed, gate_mat, up_mat):
    gate_pre = jnp.dot(normed, gate_mat, preferred_element_type=F32)
    up_pre = jnp.dot(normed, up_mat, preferred_element_type=F32)
    return gate_pre, up_pre


def outputs(gate_pre, up_pre, weight, down_mat):
    activated = (gate_pre * jax.nn.sigmoid(gate_pre) * up_pre).astype(BF16)
    out = jnp.dot(activated, down_mat, preferred_element_type=F32)
    return (out * weight).astype(BF16)


def pullback(gate_pre, up_pre, scale, inverse, rows, down_mat):
    back = lax.dot_general(rows, down_mat, (((1,), (1,)), ((), ())), preferred_element_type=F32) * scale
    sigma = jax.nn.sigmoid(gate_pre)
    grad_gate = back * up_pre * sigma * (1.0 + gate_pre * (1.0 - sigma))
    grad_up = back * gate_pre * sigma
    share = jnp.sum(grad_gate * gate_pre + grad_up * up_pre, axis=1)
    return jnp.sum(grad_gate * inverse, axis=0), jnp.sum(grad_up * inverse, axis=0), share


def token_weights(routes, gate_probs, experts):
    named = routes[:, :, None] == jnp.arange(experts, dtype=jnp.int32)
    return jnp.sum(jnp.where(named, gate_probs[:, :, None], 0.0), axis=1)


def fast_body(hidden, steering, norm_gain, target, routes, gate_probs, contrast, gate_weight, up_weight, down_weight):
    tokens, half = hidden.shape
    devices = 2 * lax.axis_size("dp")
    experts = lax.axis_size("dp")
    full = 2 * half
    gate_mat, up_mat, down_mat = gate_weight[0], up_weight[0], down_weight[0]
    here, side = lax.axis_index("dp"), lax.axis_index("mp")
    even = here % 2 == 0
    low_side = side == 0
    top = devices.bit_length() - 1
    order = [1 << 2] + [1 << b for b in range(top - 1, 2, -1)] + [1]
    orders = (order, order[1:] + order[:1])
    steps = len(order)

    def hop(value, step):
        pairs = [(i, i ^ orders[(i >> 1) & 1][step]) for i in range(devices)]
        return lax.ppermute(value, BOTH, pairs)

    def swap(value):
        return lax.ppermute(value, BOTH, [(i, i ^ 2) for i in range(devices)])

    def cross(value):
        return lax.ppermute(value, BOTH, [(i, i ^ 1) for i in range(devices)])

    def spread(value):
        held = value
        for step in range(steps - 2):
            held = jnp.concatenate([held, hop(held, step)], axis=0)
        q01 = hop(held, steps - 2)
        q10 = hop(held, steps - 1)
        q11 = hop(q01, steps - 1)
        own = jnp.concatenate([held, jnp.where(even, q01, q10)], axis=0)
        other = jnp.concatenate([jnp.where(even, q10, q01), q11], axis=0)
        return own, other

    def natural(own, other):
        return jnp.concatenate([jnp.where(low_side, own, other), jnp.where(low_side, other, own)], axis=1)

    gain = norm_gain.astype(F32)
    sign = (2 * contrast - 1).astype(F32)
    weights = token_weights(routes, gate_probs, experts)
    meta = jnp.concatenate([*thirds(weights), sign.astype(BF16)[:, None]], axis=1)
    pad = -meta.shape[1] % 128
    meta = jnp.pad(meta, ((0, 0), (0, pad)))
    vectors = jnp.stack([steering, gain])
    vectors_other = cross(vectors)
    steer_row, gain_row = natural(vectors, vectors_other)[:, None, :]

    own, other = spread(jnp.concatenate([hidden, meta], axis=1))
    info = own[:, half:].astype(F32)
    stream = natural(own[:, :half], other[:, :half]).astype(F32) + steer_row
    inverse = lax.rsqrt(jnp.mean(stream * stream, axis=1, keepdims=True) + EPSILON)
    normed = (stream * inverse * gain_row).astype(BF16)
    mine = jnp.stack([info[:, here + k * experts] for k in range(3)]).sum(axis=0)
    theirs = jnp.stack([info[:, (here ^ 1) + k * experts] for k in range(3)]).sum(axis=0)
    row_sign = info[:, 3 * experts]
    normed_far = swap(normed)
    facts_far = swap(jnp.stack([theirs, row_sign, inverse[:, 0]]))
    weight_near = mine[:, None]
    scale_near = (mine * row_sign)[:, None]
    weight_far = facts_far[0][:, None]
    scale_far = (facts_far[0] * facts_far[1])[:, None]
    inverse_far = facts_far[2][:, None]

    gate_near, up_near = forward(normed, gate_mat, up_mat)
    gate_far, up_far = forward(normed_far, gate_mat, up_mat)
    out_far = outputs(gate_far, up_far, weight_far, down_mat)
    out_here = swap(out_far)
    out_near = outputs(gate_near, up_near, weight_near, down_mat)

    rows = out_near.shape[0] // 2
    total = (out_near.astype(F32) + out_here.astype(F32)).astype(BF16)
    own = jnp.where(low_side, total[:, :half], total[:, half:])
    other = jnp.where(low_side, total[:, half:], total[:, :half])
    q00, q11 = own[:rows], other[rows:]
    q01 = jnp.where(even, own[rows:], other[:rows])
    q10 = jnp.where(even, other[:rows], own[rows:])

    def add(addends, low, high):
        return sum(a[low:high].astype(F32) for a in addends)

    from11 = hop(q11, steps - 1)
    from10 = hop(q10, steps - 1)
    addends = [q00, from10, hop(add([q01, from11], 0, rows).astype(BF16), steps - 2)]
    for step in range(steps - 3, -1, -1):
        rows //= 2
        addends.append(hop(add(addends, rows, 2 * rows).astype(BF16), step))
    out_tok = add(addends, 0, tokens)
    mixed = (hidden.astype(F32) + steering[None, :] + out_tok).astype(BF16)

    target_near = natural(*spread(target))
    target_far = swap(target_near)
    vg0, vu0, share0 = pullback(gate_near, up_near, scale_near, inverse, target_near, down_mat)
    vg1, vu1, share1 = pullback(gate_far, up_far, scale_far, inverse_far, target_far, down_mat)
    through = rows_times(vg0 + vg1, gate_mat, 1) + rows_times(vu0 + vu1, up_mat, 1)
    along = rows_times(share0 * inverse[:, 0], normed, 0) + rows_times(share1 * inverse_far[:, 0], normed_far, 0)
    partial = gain_row[0] * through - along / (gain_row[0] * full)
    low_part, high_part = partial[:half], partial[half:]
    grad = jnp.where(low_side, low_part, high_part) + cross(jnp.where(low_side, high_part, low_part))
    grad = grad + jnp.sum(target.astype(F32) * sign[:, None], axis=0)
    grad = grad + swap(grad)
    for bit in range(2, top):
        grad = grad + lax.ppermute(grad, BOTH, [(i, i ^ (1 << bit)) for i in range(devices)])
    return mixed, grad


def general_body(hidden, steering, norm_gain, target, routes, gate_probs, contrast, gate_weight, up_weight, down_weight):
    tokens, width = hidden.shape
    groups, parts = lax.axis_size("dp"), lax.axis_size("mp")
    local_experts = gate_weight.shape[0]
    full = width * parts
    here, side = lax.axis_index("dp"), lax.axis_index("mp")

    def gather(value):
        return lax.all_gather(lax.all_gather(value, "mp", axis=1, tiled=True), "dp", axis=0, tiled=True)

    sign = (2 * contrast - 1).astype(F32)
    weights = token_weights(routes, gate_probs, local_experts * groups)
    facts = lax.all_gather(jnp.concatenate([weights, sign[:, None]], axis=1), "dp", axis=0, tiled=True)
    steer_row = lax.all_gather(steering, "mp", axis=0, tiled=True)[None, :]
    gain_row = lax.all_gather(norm_gain.astype(F32), "mp", axis=0, tiled=True)[None, :]
    stream = gather(hidden).astype(F32) + steer_row
    inverse = lax.rsqrt(jnp.mean(stream * stream, axis=1, keepdims=True) + EPSILON)
    normed = (stream * inverse * gain_row).astype(BF16)
    all_target = gather(target)
    out, through, share = 0.0, 0.0, 0.0
    for k in range(local_experts):
        weight = lax.dynamic_index_in_dim(facts, here * local_experts + k, axis=1)
        gate_pre, up_pre = forward(normed, gate_weight[k], up_weight[k])
        out = out + outputs(gate_pre, up_pre, weight, down_weight[k]).astype(F32)
        vg, vu, part = pullback(gate_pre, up_pre, weight * facts[:, -1:], inverse, all_target, down_weight[k])
        through = through + rows_times(vg, gate_weight[k], 1) + rows_times(vu, up_weight[k], 1)
        share = share + part
    out = lax.psum_scatter(out.astype(BF16), "mp", scatter_dimension=1, tiled=True)
    out_tok = lax.psum_scatter(out, "dp", scatter_dimension=0, tiled=True).astype(F32)
    mixed = (hidden.astype(F32) + steering[None, :] + out_tok).astype(BF16)
    along = rows_times(share * inverse[:, 0], normed, 0)
    partial = gain_row[0] * through - along / (gain_row[0] * full)
    own = jnp.sum(target.astype(F32) * sign[:, None], axis=0)
    grad = lax.psum(partial, "mp")
    grad = lax.dynamic_slice_in_dim(grad, side * width, width) + own
    return mixed, lax.psum(grad, "dp")


def solution(mesh):
    groups, parts = mesh.shape["dp"], mesh.shape["mp"]
    fast = parts == 2 and groups >= 8 and groups & (groups - 1) == 0

    def body(*args):
        if fast and args[7].shape[0] == 1:
            return fast_body(*args)
        return general_body(*args)

    placed = (
        P("dp", "mp"),
        P("mp"),
        P("mp"),
        P("dp", "mp"),
        P("dp", None),
        P("dp", None),
        P("dp"),
        P("dp", None, "mp"),
        P("dp", None, "mp"),
        P("dp", "mp", None),
    )
    return jax.shard_map(
        body, mesh=mesh, in_specs=placed, out_specs=(P("dp", "mp"), P("mp")), check_vma=False
    )
```

```python
import jax
import jax.numpy as jnp
from jax import lax
from jax.experimental import pallas as pl
from jax.experimental.pallas import tpu as pltpu
from jax.sharding import PartitionSpec as P

EPSILON = 1e-06
BF16 = jnp.bfloat16
F32 = jnp.float32
BOTH = ("dp", "mp")


def thirds(values):
    high = lax.reduce_precision(values, 8, 7)
    rest = values - high
    middle = lax.reduce_precision(rest, 8, 7)
    low = rest - middle
    return high.astype(BF16), middle.astype(BF16), low.astype(BF16)


def rows_times(values, matrix, contracted):
    rows = lax.optimization_barrier(jnp.stack(thirds(values)))
    return jnp.sum(
        lax.dot_general(rows, matrix, (((1,), (contracted,)), ((), ())), preferred_element_type=F32),
        axis=0,
    )


def forward(normed, gate_mat, up_mat):
    gate_pre = jnp.dot(normed, gate_mat, preferred_element_type=F32)
    up_pre = jnp.dot(normed, up_mat, preferred_element_type=F32)
    return lax.optimization_barrier((gate_pre, up_pre))


def outputs(gate_pre, up_pre, weight, down_mat):
    activated = lax.optimization_barrier((gate_pre * jax.nn.sigmoid(gate_pre) * up_pre).astype(BF16))
    out = jnp.dot(activated, down_mat, preferred_element_type=F32)
    return (out * weight).astype(BF16)


def pullback(gate_pre, up_pre, scale, inverse, rows, down_mat):
    back = lax.dot_general(rows, down_mat, (((1,), (1,)), ((), ())), preferred_element_type=F32)
    back = lax.optimization_barrier(back) * scale
    sigma = jax.nn.sigmoid(gate_pre)
    grad_gate = back * up_pre * sigma * (1.0 + gate_pre * (1.0 - sigma))
    grad_up = back * gate_pre * sigma
    share = jnp.sum(grad_gate * gate_pre + grad_up * up_pre, axis=1)
    return jnp.sum(grad_gate * inverse, axis=0), jnp.sum(grad_up * inverse, axis=0), share


def token_weights(routes, gate_probs, experts):
    named = routes[:, :, None] == jnp.arange(experts, dtype=jnp.int32)
    return jnp.sum(jnp.where(named, gate_probs[:, :, None], 0.0), axis=1)


def after(value, *others):
    return lax.optimization_barrier((value, *others))[0]


def tile_of(size, most):
    return max(t for t in range(128, most + 1, 128) if size % t == 0)


VMEM = pl.BlockSpec(memory_space=pltpu.VMEM)
SMEM = pl.BlockSpec(memory_space=pltpu.SMEM)
ANY = pl.BlockSpec(memory_space=pltpu.HBM)


def call(kernel, operands, specs, outs, scratch, megabytes, flops, moved):
    return pl.pallas_call(
        kernel,
        in_specs=specs,
        out_specs=[VMEM] * len(outs),
        out_shape=[jax.ShapeDtypeStruct(shape, dtype) for shape, dtype in outs],
        scratch_shapes=scratch,
        compiler_params=pltpu.CompilerParams(vmem_limit_bytes=megabytes << 20),
        cost_estimate=pl.CostEstimate(flops=flops, bytes_accessed=moved, transcendentals=0),
    )(*operands)


CHUNK = 16
WEIGHT, SIGNED, SQUARES, INVERSE = 0, 1, 2, 3


def column(array, index):
    return array[:, index : index + 1]


def facts_of(columns):
    rows = columns[0].shape[0]
    lane = lax.broadcasted_iota(jnp.int32, (rows, 128), 1)
    found = jnp.zeros((rows, 128), F32)
    for index, values in enumerate(columns):
        found = jnp.where(lane == index, values, found)
    return found


def scale_rows(blocks, steer, gain, scaled, squares):
    first, half = 0, scaled.shape[1]
    for source in blocks:
        group = next(g for g in (4, 2, 1) if source.shape[0] % (g * CHUNK) == 0)

        def chunks(number, carry, source=source, first=first, group=group):
            for k in range(group):
                at = pl.multiple_of((number * group + k) * CHUNK, CHUNK)
                stream = source[pl.ds(at, CHUNK), :half].astype(F32) + steer
                scaled[pl.ds(first + at, CHUNK), :] = (stream * gain).astype(BF16)
                square = stream * stream
                squares[pl.ds(first + at, CHUNK), :] = sum(square[:, c : c + 128] for c in range(0, half, 128))
            return carry

        lax.fori_loop(0, source.shape[0] // (group * CHUNK), chunks, 0)
        first += source.shape[0]


def fetches(source, buffer, sems, view, ahead=2):
    count = buffer.shape[0]
    copies = lambda i: pltpu.make_async_copy(view(source, i), buffer.at[i], sems.at[i])
    for i in range(min(ahead, count)):
        copies(i).start()

    def take(i):
        copies(i).wait()

        @pl.when(i + ahead < count)
        def _():
            copies(i + ahead).start()

    return take


def split_dot(rows, matrix):
    middle = rows.shape[0] // 2
    return jnp.concatenate(
        [jnp.dot(rows[part, :], matrix, preferred_element_type=F32) for part in (slice(0, middle), slice(middle, None))], axis=0
    )


def half_fetches(gate_mat, up_mat, gate_buf, up_buf, gate_sems, up_sems, chosen):
    tile = gate_buf.shape[2]
    view = lambda source, i: source.at[chosen, :, pl.ds(i * tile, tile)]
    return fetches(gate_mat, gate_buf, gate_sems, view), fetches(up_mat, up_buf, up_sems, view)


def own_kernel(experts, which, a, b, c, d, steer, gain, gate_mat, up_mat, gate_acc, up_acc, scaled, facts, gate_buf, up_buf, gate_sems, up_sems, squares):
    gate_wait, up_wait = half_fetches(gate_mat, up_mat, gate_buf, up_buf, gate_sems, up_sems, which[0])
    half, tile = scaled.shape[1], gate_buf.shape[2]
    scale_rows((a, b, c, d), steer[which[0]], gain[which[0]], scaled, squares)
    first = 0
    for source in (a, b, c, d):
        rows = slice(first, first + source.shape[0])
        values = source[:, half:].astype(F32)
        lane = lax.broadcasted_iota(jnp.int32, values.shape, 1)
        mine = (lane == which[2]) | (lane == which[2] + experts) | (lane == which[2] + 2 * experts)
        weight = jnp.sum(jnp.where(mine, values, 0.0), axis=1, keepdims=True)
        sign = jnp.sum(jnp.where(lane == 3 * experts, values, 0.0), axis=1, keepdims=True)
        facts[rows, :] = facts_of([weight, weight * sign, jnp.sum(squares[rows, :], axis=1, keepdims=True)])
        first += source.shape[0]

    def step(i, carry):
        at = pl.ds(pl.multiple_of(i * tile, tile), tile)
        gate_wait(i)
        gate_acc[:, at] = split_dot(scaled, gate_buf[i])
        up_wait(i)
        up_acc[:, at] = split_dot(scaled, up_buf[i])
        return carry

    lax.fori_loop(0, gate_buf.shape[0], step, 0)


def other_kernel(which, a, b, c, d, steer, gain, gate_mat, up_mat, gate_acc, up_acc, facts, gate_pre, up_pre, activated, scaled, found, gate_buf, up_buf, gate_sems, up_sems, squares):
    gate_wait, up_wait = half_fetches(gate_mat, up_mat, gate_buf, up_buf, gate_sems, up_sems, which[1])
    half, tile = scaled.shape[1], gate_buf.shape[2]
    scale_rows((a, b, c, d), steer[which[1]], gain[which[1]], scaled, squares)
    old = facts[...]
    total = column(old, SQUARES) + jnp.sum(squares[...], axis=1, keepdims=True)
    found[...] = facts_of([column(old, WEIGHT), column(old, SIGNED), total, lax.rsqrt(total / (2 * half) + EPSILON)])

    def step(i, carry):
        at = pl.ds(pl.multiple_of(i * tile, tile), tile)
        inverse = column(found[...], INVERSE)
        gate_wait(i)
        gate = (gate_acc[:, at] + split_dot(scaled, gate_buf[i])) * inverse
        gate_pre[:, at] = gate
        up_wait(i)
        up = (up_acc[:, at] + split_dot(scaled, up_buf[i])) * inverse
        up_pre[:, at] = up
        activated[:, at] = (gate * jax.nn.sigmoid(gate) * up).astype(BF16)
        return carry

    lax.fori_loop(0, gate_buf.shape[0], step, 0)


def half_products(which, blocks, steer, gain, gate_mat, up_mat, state=None):
    half, units = gate_mat.shape[1:]
    rows, tile = sum(b.shape[0] for b in blocks), tile_of(units, 256)
    unit, wide = ((rows, units), F32), ((rows, half), BF16)
    facts = (rows, 128), F32
    buffer, sems = pltpu.VMEM((units // tile, half, tile), BF16), pltpu.SemaphoreType.DMA((units // tile,))
    operands = [which, *blocks, steer, gain, gate_mat, up_mat]
    specs = [SMEM] + [VMEM] * 6 + [ANY] * 2
    if state is None:
        experts = lax.axis_size("dp")
        kernel = lambda *refs: own_kernel(experts, *refs)
        outs = [unit, unit, wide, facts]
    else:
        kernel = other_kernel
        operands += state
        specs += [VMEM] * 3
        outs = [unit, unit, ((rows, units), BF16), wide, facts]
    return call(
        kernel,
        operands,
        specs,
        outs,
        [buffer, buffer, sems, sems, pltpu.VMEM((rows, 128), F32)],
        44,
        4 * rows * half * units,
        4 * half * units,
    )


def out_kernel(chosen, which, activated, facts, down_mat, near, far, buf, sems):
    tile, height = buf.shape[2], near.shape[0]
    tiles = buf.shape[0]
    start = which[chosen] * (tile * tiles)
    wait = fetches(down_mat, buf, sems, lambda source, i: source.at[:, pl.ds(pl.multiple_of(start + i * tile, tile), tile)], 3)

    def step(i, carry):
        at = pl.ds(pl.multiple_of(i * tile, tile), tile)
        wait(i)
        out = split_dot(activated, buf[i]) * column(facts[...], WEIGHT)
        near[:, at] = out[:height].astype(BF16)
        far[:, at] = out[height:].astype(BF16)
        return carry

    lax.fori_loop(0, tiles, step, 0)


def expert_out(chosen, which, activated, facts, down_mat):
    rows, units = activated.shape
    half = down_mat.shape[1] // 2
    tile = tile_of(half, 512)
    out = ((rows // 2, half), BF16)
    return call(
        lambda *refs: out_kernel(chosen, *refs),
        (which, activated, facts, down_mat),
        [SMEM, VMEM, VMEM, ANY],
        [out, out],
        [pltpu.VMEM((half // tile, units, tile), BF16), pltpu.SemaphoreType.DMA((half // tile,))],
        44,
        2 * rows * half * units,
        2 * half * units,
    )


def back_kernel(which, near_own, far_own, near_other, far_other, gate_pre, up_pre, facts, down_mat, gate_sum, up_sum, share, own_buf, other_buf, own_sems, other_sems):
    tile, half = own_buf.shape[1:]
    view = lambda h: lambda source, i: source.at[pl.ds(i * tile, tile), pl.ds(pl.multiple_of(which[h] * half, half), half)]
    own_take = fetches(down_mat, own_buf, own_sems, view(0))
    other_take = fetches(down_mat, other_buf, other_sems, view(1))
    dims = (((1,), (1,)), ((), ()))
    share[...] = jnp.zeros_like(share)
    height = near_own.shape[0]

    def step(i, carry):
        at = pl.ds(pl.multiple_of(i * tile, tile), tile)
        own_take(i)
        other_take(i)
        gate_total, up_total = 0.0, 0.0
        for first, own, other in ((0, near_own, near_other), (height, far_own, far_other)):
            rows = slice(first, first + height)
            known = facts[rows, :]
            back = lax.dot_general(own[...], own_buf[i], dims, preferred_element_type=F32)
            back += lax.dot_general(other[...], other_buf[i], dims, preferred_element_type=F32)
            back *= column(known, SIGNED)
            gate, up = gate_pre[rows, at], up_pre[rows, at]
            sigma = jax.nn.sigmoid(gate)
            grad_gate = back * up * sigma * (1.0 + gate * (1.0 - sigma))
            grad_up = back * gate * sigma
            inverse = column(known, INVERSE)
            gate_total += jnp.sum(grad_gate * inverse, axis=0, keepdims=True)
            up_total += jnp.sum(grad_up * inverse, axis=0, keepdims=True)
            part = grad_gate * gate + grad_up * up
            share[rows, :] += sum(part[:, c : c + 128] for c in range(0, tile, 128))
        gate_sum[:, at] = gate_total
        up_sum[:, at] = up_total
        return carry

    lax.fori_loop(0, own_buf.shape[0], step, 0)


def expert_back(which, rows_of, down_mat, gate_pre, up_pre, facts):
    half = rows_of[0].shape[1]
    rows, units = gate_pre.shape
    tile = tile_of(units, 256)
    buffer, sems = pltpu.VMEM((units // tile, tile, half), BF16), pltpu.SemaphoreType.DMA((units // tile,))
    return call(
        back_kernel,
        (which, *rows_of, gate_pre, up_pre, facts, down_mat),
        [SMEM] + [VMEM] * 7 + [ANY],
        [((1, units), F32), ((1, units), F32), ((rows, 128), F32)],
        [buffer, buffer, sems, sems],
        44,
        4 * rows * half * units,
        4 * half * units,
    )


def through_kernel(gate_sum, up_sum, gate_mat, up_mat, out, gate_buf, up_buf, gate_sems, up_sems):
    tiles, tile, units = gate_buf.shape
    view = lambda source, i: source.at[pl.ds(i * tile, tile), :]
    gate_wait = fetches(gate_mat, gate_buf, gate_sems, view)
    up_wait = fetches(up_mat, up_buf, up_sems, view)
    chunk = 128

    def step(i, carry):
        gate_wait(i)
        up_wait(i)

        for r in range(tile // chunk):
            at = pl.ds(r * chunk, chunk)
            total = jnp.zeros((chunk, 128), F32)
            for c in range(0, units, 128):
                lanes = slice(c, c + 128)
                total += gate_buf[i, at, lanes].astype(F32) * gate_sum[:, lanes]
                total += up_buf[i, at, lanes].astype(F32) * up_sum[:, lanes]
            to = pl.ds(pl.multiple_of(i * tile + r * chunk, chunk), chunk)
            out[:, to] = jnp.sum(total.T, axis=0, keepdims=True)
        return carry

    lax.fori_loop(0, tiles, step, 0)


def through_weights(gate_sum, up_sum, gate_mat, up_mat):
    full, units = gate_mat.shape
    tile = tile_of(full, 896)
    buffer, sems = pltpu.VMEM((full // tile, tile, units), BF16), pltpu.SemaphoreType.DMA((full // tile,))
    return call(
        through_kernel,
        (gate_sum, up_sum, gate_mat, up_mat),
        [VMEM, VMEM, ANY, ANY],
        [((1, full), F32)],
        [buffer, buffer, sems, sems],
        48,
        512 * full * units,
        4 * full * units,
    )[0]


def fast_body(hidden, steering, norm_gain, target, routes, gate_probs, contrast, gate_weight, up_weight, down_weight):
    tokens, half = hidden.shape
    devices = 2 * lax.axis_size("dp")
    experts = lax.axis_size("dp")
    full = 2 * half
    gate_mat, up_mat, down_mat = gate_weight[0], up_weight[0], down_weight[0]
    gate_halves = gate_mat.reshape(2, half, gate_mat.shape[1])
    up_halves = up_mat.reshape(2, half, up_mat.shape[1])
    here, side = lax.axis_index("dp"), lax.axis_index("mp")
    even = here % 2 == 0
    low_side = side == 0
    which = jnp.stack([side, 1 - side, here]).astype(jnp.int32)
    top = devices.bit_length() - 1
    falling = [1 << b for b in range(top - 1, 2, -1)]
    orders = (falling + [1 << 2, 1], [1 << 2] + falling[:-1] + [1, falling[-1]])
    steps = len(falling) + 2
    last, third = steps - 1, steps - 2

    def permute(value, mask):
        return lax.ppermute(value, BOTH, [(i, i ^ mask(i)) for i in range(devices)])

    def hop(value, step):
        return permute(value, lambda i: orders[(i >> 1) & 1][step])

    def swap(value):
        return permute(value, lambda i: 2)

    def cross(value):
        return permute(value, lambda i: 1)

    def spread(value, gates=None):
        hold = (lambda v, g: after(v, *gates[g])) if gates else (lambda v, g: v)
        held = hold(value, 0)
        for step in range(steps - 3):
            held = jnp.concatenate([held, hop(held, step)], axis=0)
        p0 = hold(held, 1)
        p1 = hop(p0, steps - 3)
        p4 = hop(p0, last)
        p2 = hop(p0, third)
        p1, p2 = hold(p1, 2), hold(p2, 2)
        p3 = hop(p1, third)
        p5 = hop(p1, last)
        p6 = hop(p2, last)
        p7 = hop(hold(p3, 3), last)
        join = lambda a, b: jnp.concatenate([a, b], axis=0)
        own_a = join(p0, p1)
        own_b = join(jnp.where(even, p2, p4), jnp.where(even, p3, p5))
        other_a = join(jnp.where(even, p4, p2), jnp.where(even, p5, p3))
        return [own_a, own_b, other_a, join(p6, p7)], ((p3, p5), (p6, p7))

    gain = norm_gain.astype(F32)
    sign = (2 * contrast - 1).astype(F32)
    weights = token_weights(routes, gate_probs, experts)
    meta = jnp.concatenate([*thirds(weights), sign.astype(BF16)[:, None]], axis=1)
    meta = jnp.pad(meta, ((0, 0), (0, 128 - meta.shape[1])))
    vectors = jnp.stack([steering, gain])
    vectors_other = cross(vectors)
    steer_halves = jnp.where(low_side, jnp.stack([vectors[0], vectors_other[0]]), jnp.stack([vectors_other[0], vectors[0]]))
    gain_halves = jnp.where(low_side, jnp.stack([vectors[1], vectors_other[1]]), jnp.stack([vectors_other[1], vectors[1]]))
    steer_halves, gain_halves = steer_halves[:, None, :], gain_halves[:, None, :]

    (own_a, own_b, other_a, other_b), arrived = spread(jnp.concatenate([hidden, meta], axis=1))
    shared = (steer_halves, gain_halves, gate_halves, up_halves)
    gate_acc, up_acc, own_scaled, facts = half_products(which, (own_a, own_b, swap(own_a), swap(own_b)), *shared)
    other_far_a = swap(other_a)
    other_b = after(other_b, facts)
    gate_pre, up_pre, activated, other_scaled, facts = half_products(
        which, (other_a, other_b, other_far_a, swap(other_b)), *shared, (gate_acc, up_acc, facts)
    )
    near_other, far_other = expert_out(1, which, activated, facts, down_mat)
    here_other = swap(far_other)
    near_own, far_own = expert_out(0, which, after(activated, near_other), facts, down_mat)
    here_own = swap(far_own)

    targets, _ = spread(target, (*arrived, (activated,), (near_other,)))

    def add(*addends):
        return sum(a.astype(F32) for a in addends).astype(BF16)

    rows = near_own.shape[0] // 4
    sum_own, sum_other = (near_own, here_own), (near_other, here_other)
    piece = lambda pair, i: add(*(v[i * rows : (i + 1) * rows] for v in pair))
    a7, a6 = piece(sum_other, 3), piece(sum_other, 2)
    a5 = jnp.where(even, piece(sum_other, 1), piece(sum_own, 3))
    a4 = jnp.where(even, piece(sum_other, 0), piece(sum_own, 2))
    a3 = jnp.where(even, piece(sum_own, 3), piece(sum_other, 1))
    a2 = jnp.where(even, piece(sum_own, 2), piece(sum_other, 0))
    a1, a0 = piece(sum_own, 1), piece(sum_own, 0)
    b3 = hop(a7, last)
    b2 = hop(a6, last)
    b1 = hop(a5, last)
    b0 = hop(a4, last)
    third1, third0 = add(a3, b3), add(a2, b2)
    c1 = hop(third1, third)
    c0 = hop(third0, third)
    early = add(a1, b1, c1)
    d0 = hop(early, steps - 3)
    addends = [a0, b0, c0, d0]
    for step in range(steps - 4, -1, -1):
        rows //= 2
        addends.append(hop(add(*(a[rows : 2 * rows] for a in addends)), step))
    out_tok = sum(a[:tokens].astype(F32) for a in addends)
    mixed = (hidden.astype(F32) + steering[None, :] + out_tok).astype(BF16)

    own_a, own_b, other_a, other_b = targets
    target_own = jnp.concatenate([own_a, own_b], axis=0)
    target_other = jnp.concatenate([other_a, other_b], axis=0)
    far = swap(target_own), swap(target_other)
    rows_of = after(target_own, a7, a6, a5, a4), far[0], target_other, far[1]
    gate_sum, up_sum, share = expert_back(which, rows_of, down_mat, gate_pre, up_pre, facts)
    through = through_weights(after(gate_sum, third1, third0), up_sum, gate_mat, up_mat)[0]
    along = jnp.sum(after(share, early), axis=1) * facts[:, INVERSE] * facts[:, INVERSE]
    along_own, along_other = rows_times(along, own_scaled, 0), rows_times(along, other_scaled, 0)
    low_part, high_part = through[:half], through[half:]
    through_own = jnp.where(low_side, low_part, high_part)
    through_other = jnp.where(low_side, high_part, low_part)
    finish = lambda through, along, gain: gain * through - along / (gain * full)
    grad = finish(through_own, along_own, gain) + cross(finish(through_other, along_other, vectors_other[1]))
    grad = grad + jnp.sum(target.astype(F32) * sign[:, None], axis=0)
    bits = [1 << bit for bit in range(1, top)]
    for group in (bits[:2], bits[2:4], *([bit] for bit in bits[4:])):
        masks = [sum(bit for k, bit in enumerate(group) if n >> k & 1) for n in range(1, 1 << len(group))]
        grad = sum([permute(grad, lambda i, mask=mask: mask) for mask in masks], grad)
    return mixed, grad


def general_body(hidden, steering, norm_gain, target, routes, gate_probs, contrast, gate_weight, up_weight, down_weight):
    _, width = hidden.shape
    groups, parts = lax.axis_size("dp"), lax.axis_size("mp")
    local_experts = gate_weight.shape[0]
    full = width * parts
    here, side = lax.axis_index("dp"), lax.axis_index("mp")

    def gather(value):
        return lax.all_gather(lax.all_gather(value, "mp", axis=1, tiled=True), "dp", axis=0, tiled=True)

    sign = (2 * contrast - 1).astype(F32)
    weights = token_weights(routes, gate_probs, local_experts * groups)
    facts = lax.all_gather(jnp.concatenate([weights, sign[:, None]], axis=1), "dp", axis=0, tiled=True)
    steer_row = lax.all_gather(steering, "mp", axis=0, tiled=True)[None, :]
    gain_row = lax.all_gather(norm_gain.astype(F32), "mp", axis=0, tiled=True)[None, :]
    stream = gather(hidden).astype(F32) + steer_row
    inverse = lax.rsqrt(jnp.mean(stream * stream, axis=1, keepdims=True) + EPSILON)
    normed = (stream * inverse * gain_row).astype(BF16)
    all_target = gather(target)
    out, through, share = 0.0, 0.0, 0.0
    for k in range(local_experts):
        weight = lax.dynamic_index_in_dim(facts, here * local_experts + k, axis=1)
        gate_pre, up_pre = forward(normed, gate_weight[k], up_weight[k])
        out = out + outputs(gate_pre, up_pre, weight, down_weight[k]).astype(F32)
        vg, vu, part = pullback(gate_pre, up_pre, weight * facts[:, -1:], inverse, all_target, down_weight[k])
        through = through + rows_times(vg, gate_weight[k], 1) + rows_times(vu, up_weight[k], 1)
        share = share + part
    out = lax.psum_scatter(out.astype(BF16), "mp", scatter_dimension=1, tiled=True)
    out_tok = lax.psum_scatter(out, "dp", scatter_dimension=0, tiled=True).astype(F32)
    mixed = (hidden.astype(F32) + steering[None, :] + out_tok).astype(BF16)
    along = rows_times(share * inverse[:, 0], normed, 0)
    partial = gain_row[0] * through - along / (gain_row[0] * full)
    own = jnp.sum(target.astype(F32) * sign[:, None], axis=0)
    grad = lax.psum(partial, "mp")
    grad = lax.dynamic_slice_in_dim(grad, side * width, width) + own
    return mixed, lax.psum(grad, "dp")


def solution(mesh):
    groups, parts = mesh.shape["dp"], mesh.shape["mp"]
    fast = parts == 2 and 8 <= groups <= 32 and groups & (groups - 1) == 0

    def body(*args):
        if fast and args[7].shape[0] == 1:
            return fast_body(*args)
        return general_body(*args)

    placed = (
        P("dp", "mp"),
        P("mp"),
        P("mp"),
        P("dp", "mp"),
        P("dp", None),
        P("dp", None),
        P("dp"),
        P("dp", None, "mp"),
        P("dp", None, "mp"),
        P("dp", "mp", None),
    )
    return jax.shard_map(
        body, mesh=mesh, in_specs=placed, out_specs=(P("dp", "mp"), P("mp")), check_vma=False
    )
```

```python
import jax
import jax.numpy as jnp
from jax import lax
from jax.experimental import pallas as pl
from jax.experimental.pallas import tpu as pltpu
from jax.sharding import PartitionSpec as P

EPSILON = 1e-06
BF16 = jnp.bfloat16
F32 = jnp.float32
BOTH = ("dp", "mp")


def thirds(values):
    high = lax.reduce_precision(values, 8, 7)
    rest = values - high
    middle = lax.reduce_precision(rest, 8, 7)
    low = rest - middle
    return high.astype(BF16), middle.astype(BF16), low.astype(BF16)


def rows_times(values, matrix, contracted):
    rows = lax.optimization_barrier(jnp.stack(thirds(values)))
    return jnp.sum(
        lax.dot_general(rows, matrix, (((1,), (contracted,)), ((), ())), preferred_element_type=F32),
        axis=0,
    )


def forward(normed, gate_mat, up_mat):
    gate_pre = jnp.dot(normed, gate_mat, preferred_element_type=F32)
    up_pre = jnp.dot(normed, up_mat, preferred_element_type=F32)
    return lax.optimization_barrier((gate_pre, up_pre))


def outputs(gate_pre, up_pre, weight, down_mat):
    activated = lax.optimization_barrier((gate_pre * jax.nn.sigmoid(gate_pre) * up_pre).astype(BF16))
    out = jnp.dot(activated, down_mat, preferred_element_type=F32)
    return (out * weight).astype(BF16)


def pullback(gate_pre, up_pre, scale, inverse, rows, down_mat):
    back = lax.dot_general(rows, down_mat, (((1,), (1,)), ((), ())), preferred_element_type=F32)
    back = lax.optimization_barrier(back) * scale
    sigma = jax.nn.sigmoid(gate_pre)
    grad_gate = back * up_pre * sigma * (1.0 + gate_pre * (1.0 - sigma))
    grad_up = back * gate_pre * sigma
    share = jnp.sum(grad_gate * gate_pre + grad_up * up_pre, axis=1)
    return jnp.sum(grad_gate * inverse, axis=0), jnp.sum(grad_up * inverse, axis=0), share


def token_weights(routes, gate_probs, experts):
    named = routes[:, :, None] == jnp.arange(experts, dtype=jnp.int32)
    return jnp.sum(jnp.where(named, gate_probs[:, :, None], 0.0), axis=1)


def after(value, *others):
    return lax.optimization_barrier((value, *others))[0]


def tile_of(size, most):
    return max(t for t in range(128, most + 1, 128) if size % t == 0)


VMEM = pl.BlockSpec(memory_space=pltpu.VMEM)
SMEM = pl.BlockSpec(memory_space=pltpu.SMEM)
ANY = pl.BlockSpec(memory_space=pltpu.HBM)


def call(kernel, operands, specs, outs, scratch, megabytes, flops, moved):
    return pl.pallas_call(
        kernel,
        in_specs=specs,
        out_specs=[VMEM] * len(outs),
        out_shape=[jax.ShapeDtypeStruct(shape, dtype) for shape, dtype in outs],
        scratch_shapes=scratch,
        compiler_params=pltpu.CompilerParams(vmem_limit_bytes=megabytes << 20),
        cost_estimate=pl.CostEstimate(flops=flops, bytes_accessed=moved, transcendentals=0),
    )(*operands)


CHUNK = 16
WEIGHT, SIGNED, SQUARES, INVERSE = 0, 1, 2, 3


def column(array, index):
    return array[:, index : index + 1]


def facts_of(columns):
    rows = columns[0].shape[0]
    lane = lax.broadcasted_iota(jnp.int32, (rows, 128), 1)
    found = jnp.zeros((rows, 128), F32)
    for index, values in enumerate(columns):
        found = jnp.where(lane == index, values, found)
    return found


def scale_rows(blocks, steer, gain, scaled, squares):
    first, half = 0, scaled.shape[1]
    for source in blocks:
        group = next(g for g in (4, 2, 1) if source.shape[0] % (g * CHUNK) == 0)

        def chunks(number, carry, source=source, first=first, group=group):
            for k in range(group):
                at = pl.multiple_of((number * group + k) * CHUNK, CHUNK)
                stream = source[pl.ds(at, CHUNK), :half].astype(F32) + steer
                scaled[pl.ds(first + at, CHUNK), :] = (stream * gain).astype(BF16)
                square = stream * stream
                squares[pl.ds(first + at, CHUNK), :] = sum(square[:, c : c + 128] for c in range(0, half, 128))
            return carry

        lax.fori_loop(0, source.shape[0] // (group * CHUNK), chunks, 0)
        first += source.shape[0]


def fetches(source, buffer, sems, view, ahead=2):
    count, slots = sems.shape[0], buffer.shape[0]
    copies = lambda i: pltpu.make_async_copy(view(source, i), buffer.at[lax.rem(i, slots)], sems.at[i])
    for i in range(min(ahead, count)):
        copies(i).start()

    def take(i):
        copies(i).wait()

        @pl.when(i + ahead < count)
        def _():
            copies(i + ahead).start()

    return take


def split_dot(rows, matrix):
    middle = rows.shape[0] // 2
    return jnp.concatenate(
        [jnp.dot(rows[part, :], matrix, preferred_element_type=F32) for part in (slice(0, middle), slice(middle, None))], axis=0
    )


def half_fetches(gate_mat, up_mat, gate_buf, up_buf, gate_sems, up_sems, chosen):
    tile = gate_buf.shape[2]
    view = lambda source, i: source.at[chosen, :, pl.ds(i * tile, tile)]
    return fetches(gate_mat, gate_buf, gate_sems, view), fetches(up_mat, up_buf, up_sems, view)


def own_kernel(experts, which, a, b, steer, gain, gate_mat, up_mat, gate_acc, up_acc, scaled, facts, gate_buf, up_buf, gate_sems, up_sems, squares):
    gate_wait, up_wait = half_fetches(gate_mat, up_mat, gate_buf, up_buf, gate_sems, up_sems, which[0])
    half, tile = scaled.shape[1], gate_buf.shape[2]
    scale_rows((a, b), steer[which[0]], gain[which[0]], scaled, squares)
    first = 0
    for source in (a, b):
        rows = slice(first, first + source.shape[0])
        values = source[:, half:].astype(F32)
        lane = lax.broadcasted_iota(jnp.int32, values.shape, 1)
        mine = (lane == which[2]) | (lane == which[2] + experts) | (lane == which[2] + 2 * experts)
        weight = jnp.sum(jnp.where(mine, values, 0.0), axis=1, keepdims=True)
        sign = jnp.sum(jnp.where(lane == 3 * experts, values, 0.0), axis=1, keepdims=True)
        facts[rows, :] = facts_of([weight, weight * sign, jnp.sum(squares[rows, :], axis=1, keepdims=True)])
        first += source.shape[0]

    def step(i, carry):
        at = pl.ds(pl.multiple_of(i * tile, tile), tile)
        gate_wait(i)
        gate_acc[:, at] = split_dot(scaled, gate_buf[i])
        up_wait(i)
        up_acc[:, at] = split_dot(scaled, up_buf[i])
        return carry

    lax.fori_loop(0, gate_buf.shape[0], step, 0)


def other_kernel(which, a, b, c, d, steer, gain, gate_mat, up_mat, *refs):
    states, outs, scratch = (refs[0:3], refs[3:6]), (refs[6:11], refs[11:16]), refs[16:]
    gate_buf, up_buf, gate_sems, up_sems, squares = scratch
    gate_wait, up_wait = half_fetches(gate_mat, up_mat, gate_buf, up_buf, gate_sems, up_sems, which[1])
    half, tile = a.shape[1] - 128, gate_buf.shape[2]
    for blocks, state, out in zip(((a, b), (c, d)), states, outs):
        scaled, found, old = out[3], out[4], state[2][...]
        scale_rows(blocks, steer[which[1]], gain[which[1]], scaled, squares)
        total = column(old, SQUARES) + jnp.sum(squares[...], axis=1, keepdims=True)
        found[...] = facts_of([column(old, WEIGHT), column(old, SIGNED), total, lax.rsqrt(total / (2 * half) + EPSILON)])

    def step(i, carry):
        at = pl.ds(pl.multiple_of(i * tile, tile), tile)
        gate_wait(i)
        for (gate_acc, _, _), (gate_pre, _, _, scaled, found) in zip(states, outs):
            gate = gate_acc[:, at] + jnp.dot(scaled[...], gate_buf[i], preferred_element_type=F32)
            gate_pre[:, at] = gate * column(found[...], INVERSE)
        up_wait(i)
        for (_, up_acc, _), (gate_pre, up_pre, activated, scaled, found) in zip(states, outs):
            up = up_acc[:, at] + jnp.dot(scaled[...], up_buf[i], preferred_element_type=F32)
            up, gate = up * column(found[...], INVERSE), gate_pre[:, at]
            up_pre[:, at] = up
            activated[:, at] = (gate * jax.nn.sigmoid(gate) * up).astype(BF16)
        return carry

    lax.fori_loop(0, gate_buf.shape[0], step, 0)


def half_products(which, blocks, steer, gain, gate_mat, up_mat, states=()):
    half, units = gate_mat.shape[1:]
    rows, tile = 2 * blocks[0].shape[0], tile_of(units, 256)
    unit, wide, facts = ((rows, units), F32), ((rows, half), BF16), ((rows, 128), F32)
    buffer, sems = pltpu.VMEM((units // tile, half, tile), BF16), pltpu.SemaphoreType.DMA((units // tile,))
    operands = [which, *blocks, steer, gain, gate_mat, up_mat, *(v for state in states for v in state)]
    specs = [SMEM] + [VMEM] * (len(blocks) + 2) + [ANY] * 2 + [VMEM] * (3 * len(states))
    if states:
        kernel = other_kernel
        outs = [unit, unit, ((rows, units), BF16), wide, facts] * 2
    else:
        experts = lax.axis_size("dp")
        kernel = lambda *refs: own_kernel(experts, *refs)
        outs = [unit, unit, wide, facts]
    return call(
        kernel,
        operands,
        specs,
        outs,
        [buffer, buffer, sems, sems, pltpu.VMEM((rows, 128), F32)],
        44,
        2 * len(blocks) * rows * half * units,
        4 * half * units,
    )


def out_kernel(chosen, which, act_a, act_b, facts_a, facts_b, down_mat, near, far, buf, sems):
    tiles, _, tile = buf.shape
    height = act_a.shape[0] // 2
    start = which[chosen] * (tile * tiles)
    take = fetches(down_mat, buf, sems, lambda source, i: source.at[:, pl.ds(pl.multiple_of(start + i * tile, tile), tile)], 3)

    def step(i, carry):
        at = pl.ds(pl.multiple_of(i * tile, tile), tile)
        take(i)
        for first, activated, facts in ((0, act_a, facts_a), (height, act_b, facts_b)):
            out = jnp.dot(activated[...], buf[i], preferred_element_type=F32) * column(facts[...], WEIGHT)
            near[first : first + height, at] = out[:height].astype(BF16)
            far[first : first + height, at] = out[height:].astype(BF16)
        return carry

    lax.fori_loop(0, tiles, step, 0)


def expert_out(chosen, which, acts, facts, down_mat):
    rows, units = acts[0].shape
    half = down_mat.shape[1] // 2
    tile = tile_of(half, 512)
    out = ((rows, half), BF16)
    return call(
        lambda *refs: out_kernel(chosen, *refs),
        (which, *acts, *facts, down_mat),
        [SMEM] + [VMEM] * 4 + [ANY],
        [out, out],
        [pltpu.VMEM((half // tile, units, tile), BF16), pltpu.SemaphoreType.DMA((half // tile,))],
        44,
        4 * rows * half * units,
        2 * half * units,
    )


def back_kernel(which, near_own, far_own, near_other, far_other, gate_a, gate_b, up_a, up_b, facts_a, facts_b, down_mat, gate_sum, up_sum, share_a, share_b, own_buf, other_buf, own_sems, other_sems):
    tile, half = own_buf.shape[1:]
    view = lambda h: lambda source, i: source.at[pl.ds(i * tile, tile), pl.ds(pl.multiple_of(which[h] * half, half), half)]
    own_take = fetches(down_mat, own_buf, own_sems, view(0))
    other_take = fetches(down_mat, other_buf, other_sems, view(1))
    dims = (((1,), (1,)), ((), ()))
    share_a[...] = jnp.zeros_like(share_a)
    share_b[...] = jnp.zeros_like(share_b)
    height = near_own.shape[0] // 2
    groups = ((gate_a, up_a, facts_a, share_a), (gate_b, up_b, facts_b, share_b))

    def step(i, carry):
        at = pl.ds(pl.multiple_of(i * tile, tile), tile)
        own_take(i)
        other_take(i)
        gate_total, up_total = 0.0, 0.0
        for first, own, other in ((0, near_own, near_other), (height, far_own, far_other)):
            product = lax.dot_general(own[...], own_buf[i], dims, preferred_element_type=F32)
            product += lax.dot_general(other[...], other_buf[i], dims, preferred_element_type=F32)
            rows = slice(first, first + height)
            for number, (gate_pre, up_pre, facts, share) in enumerate(groups):
                known = facts[rows, :]
                back = product[number * height : (number + 1) * height] * column(known, SIGNED)
                gate, up = gate_pre[rows, at], up_pre[rows, at]
                sigma = jax.nn.sigmoid(gate)
                grad_gate = back * up * sigma * (1.0 + gate * (1.0 - sigma))
                grad_up = back * gate * sigma
                inverse = column(known, INVERSE)
                gate_total += jnp.sum(grad_gate * inverse, axis=0, keepdims=True)
                up_total += jnp.sum(grad_up * inverse, axis=0, keepdims=True)
                part = grad_gate * gate + grad_up * up
                share[rows, :] += sum(part[:, c : c + 128] for c in range(0, tile, 128))
        gate_sum[:, at] = gate_total
        up_sum[:, at] = up_total
        return carry

    lax.fori_loop(0, own_buf.shape[0], step, 0)


def expert_back(which, rows_of, down_mat, gate_pre, up_pre, facts):
    half = rows_of[0].shape[1]
    rows, units = gate_pre[0].shape
    tile = tile_of(units, 256)
    buffer, sems = pltpu.VMEM((units // tile, tile, half), BF16), pltpu.SemaphoreType.DMA((units // tile,))
    return call(
        back_kernel,
        (which, *rows_of, *gate_pre, *up_pre, *facts, down_mat),
        [SMEM] + [VMEM] * 10 + [ANY],
        [((1, units), F32), ((1, units), F32), ((rows, 128), F32), ((rows, 128), F32)],
        [buffer, buffer, sems, sems],
        44,
        8 * rows * half * units,
        4 * half * units,
    )


def through_kernel(gate_sum, up_sum, gate_mat, up_mat, out, gate_buf, up_buf, gate_sems, up_sems):
    slots, tile, units = gate_buf.shape
    view = lambda source, i: source.at[pl.ds(i * tile, tile), :]
    gate_wait = fetches(gate_mat, gate_buf, gate_sems, view)
    up_wait = fetches(up_mat, up_buf, up_sems, view)
    chunk = 128

    def step(i, carry):
        gate_wait(i)
        up_wait(i)
        slot = lax.rem(i, slots)
        for r in range(tile // chunk):
            at = pl.ds(r * chunk, chunk)
            total = jnp.zeros((chunk, 128), F32)
            for c in range(0, units, 128):
                lanes = slice(c, c + 128)
                total += gate_buf[slot, at, lanes].astype(F32) * gate_sum[:, lanes]
                total += up_buf[slot, at, lanes].astype(F32) * up_sum[:, lanes]
            to = pl.ds(pl.multiple_of(i * tile + r * chunk, chunk), chunk)
            out[:, to] = jnp.sum(total.T, axis=0, keepdims=True)
        return carry

    lax.fori_loop(0, gate_sems.shape[0], step, 0)


def through_weights(gate_sum, up_sum, gate_mat, up_mat):
    full, units = gate_mat.shape
    tile = tile_of(full, 896)
    buffer, sems = pltpu.VMEM((4, tile, units), BF16), pltpu.SemaphoreType.DMA((full // tile,))
    return call(
        through_kernel,
        (gate_sum, up_sum, gate_mat, up_mat),
        [VMEM, VMEM, ANY, ANY],
        [((1, full), F32)],
        [buffer, buffer, sems, sems],
        44,
        512 * full * units,
        4 * full * units,
    )[0]


def fast_body(hidden, steering, norm_gain, target, routes, gate_probs, contrast, gate_weight, up_weight, down_weight):
    tokens, half = hidden.shape
    devices = 2 * lax.axis_size("dp")
    experts = lax.axis_size("dp")
    full = 2 * half
    gate_mat, up_mat, down_mat = gate_weight[0], up_weight[0], down_weight[0]
    gate_halves = gate_mat.reshape(2, half, gate_mat.shape[1])
    up_halves = up_mat.reshape(2, half, up_mat.shape[1])
    here, side = lax.axis_index("dp"), lax.axis_index("mp")
    even = here % 2 == 0
    low_side = side == 0
    which = jnp.stack([side, 1 - side, here]).astype(jnp.int32)
    top = devices.bit_length() - 1
    falling = [1 << b for b in range(top - 1, 2, -1)]
    orders = (falling + [1 << 2, 1], [1 << 2] + falling[:-1] + [1, falling[-1]])
    steps = len(falling) + 2
    last, third = steps - 1, steps - 2

    def permute(value, mask):
        return lax.ppermute(value, BOTH, [(i, i ^ mask(i)) for i in range(devices)])

    def hop(value, step):
        return permute(value, lambda i: orders[(i >> 1) & 1][step])

    def swap(value):
        return permute(value, lambda i: 2)

    def cross(value):
        return permute(value, lambda i: 1)

    def spread(value, gates=None):
        hold = (lambda v, g: after(v, *gates[g])) if gates else (lambda v, g: v)
        held = hold(value, 0)
        for step in range(steps - 3):
            held = jnp.concatenate([held, hop(held, step)], axis=0)
        p0 = hold(held, 1)
        p1 = hop(p0, steps - 3)
        p4 = hop(p0, last)
        p2 = hop(p0, third)
        p1, p2 = hold(p1, 2), hold(p2, 2)
        p3 = hop(p1, third)
        p5 = hop(p1, last)
        p6 = hop(p2, last)
        p7 = hop(hold(p3, 3), last)
        return p0, p1, p2, p3, p4, p5, p6, p7

    def quarters(p):
        own_b = jnp.where(even, p[2], p[4]), jnp.where(even, p[3], p[5])
        other_a = jnp.where(even, p[4], p[2]), jnp.where(even, p[5], p[3])
        return (p[0], p[1]), own_b, other_a, (p[6], p[7])

    gain = norm_gain.astype(F32)
    sign = (2 * contrast - 1).astype(F32)
    weights = token_weights(routes, gate_probs, experts)
    meta = jnp.concatenate([*thirds(weights), sign.astype(BF16)[:, None]], axis=1)
    meta = jnp.pad(meta, ((0, 0), (0, 128 - meta.shape[1])))
    vectors = jnp.stack([steering, gain])
    vectors_other = cross(vectors)
    steer_halves = jnp.where(low_side, jnp.stack([vectors[0], vectors_other[0]]), jnp.stack([vectors_other[0], vectors[0]]))
    gain_halves = jnp.where(low_side, jnp.stack([vectors[1], vectors_other[1]]), jnp.stack([vectors_other[1], vectors[1]]))
    steer_halves, gain_halves = steer_halves[:, None, :], gain_halves[:, None, :]

    pieces = spread(jnp.concatenate([hidden, meta], axis=1))
    own_a, own_b, other_a, other_b = (jnp.concatenate(pair, axis=0) for pair in quarters(pieces))
    shared = (steer_halves, gain_halves, gate_halves, up_halves)
    state_a = half_products(which, (own_a, swap(own_a)), *shared)
    far_other_a = swap(other_a)
    state_b = half_products(which, (own_b, swap(own_b)), *shared)
    split = lambda state: ((state[0], state[1], state[3]), state[2])
    (state_a, own_scaled_a), (state_b, own_scaled_b) = split(state_a), split(state_b)
    blocks = other_a, far_other_a, other_b, swap(other_b)
    done = half_products(which, blocks, *shared, (state_a, state_b))
    (gate_a, up_a, act_a, other_scaled_a, facts_a), (gate_b, up_b, act_b, other_scaled_b, facts_b) = done[:5], done[5:]
    facts = facts_a, facts_b
    near_other, far_other = expert_out(1, which, (act_a, act_b), facts, down_mat)
    here_other = swap(far_other)
    near_own, far_own = expert_out(0, which, (act_a, after(act_b, near_other)), facts, down_mat)
    here_own = swap(far_own)

    gates = (pieces[3], pieces[5]), (pieces[6], pieces[7]), (act_b,), (near_other,)
    targets = spread(target, gates)

    def add(*addends):
        return sum(a.astype(F32) for a in addends).astype(BF16)

    rows = near_own.shape[0] // 4
    sum_own, sum_other = (near_own, here_own), (near_other, here_other)
    piece = lambda pair, i: add(*(v[i * rows : (i + 1) * rows] for v in pair))
    a7, a6 = piece(sum_other, 3), piece(sum_other, 2)
    sum_own = near_own, after(here_own, a7, a6)
    a5 = jnp.where(even, piece(sum_other, 1), piece(sum_own, 3))
    a4 = jnp.where(even, piece(sum_other, 0), piece(sum_own, 2))
    a3 = jnp.where(even, piece(sum_own, 3), piece(sum_other, 1))
    a2 = jnp.where(even, piece(sum_own, 2), piece(sum_other, 0))
    a1, a0 = piece(sum_own, 1), piece(sum_own, 0)
    b3 = hop(a7, last)
    b2 = hop(a6, last)
    b1 = hop(a5, last)
    b0 = hop(a4, last)
    third1 = add(a3, b3)
    c1 = hop(third1, third)

    own_a, own_b, other_a, other_b = quarters([after(v, a7, a6, a5, a4) for v in targets])
    target_own = jnp.concatenate(own_a + own_b, axis=0)
    target_other = jnp.concatenate(other_a + other_b, axis=0)
    far = swap(target_own), swap(target_other)
    rows_of = after(target_own, third1), far[0], target_other, far[1]
    gate_sum, up_sum, share_a, share_b = expert_back(which, rows_of, down_mat, (gate_a, gate_b), (up_a, up_b), facts)
    third0 = add(after(a2, gate_sum), b2)
    c0 = hop(third0, third)
    early = add(a1, b1, c1)
    d0 = hop(early, steps - 3)
    addends = [a0, b0, c0, d0]
    for step in range(steps - 4, -1, -1):
        rows //= 2
        addends.append(hop(add(*(a[rows : 2 * rows] for a in addends)), step))
    out_tok = sum(a[:tokens].astype(F32) for a in addends)
    mixed = (hidden.astype(F32) + steering[None, :] + out_tok).astype(BF16)
    through = through_weights(after(gate_sum, third0, early), up_sum, gate_mat, up_mat)[0]
    weigh = lambda share, facts: jnp.sum(after(share, early), axis=1) * facts[:, INVERSE] * facts[:, INVERSE]
    along_a, along_b = weigh(share_a, facts_a), weigh(share_b, facts_b)
    along_own = rows_times(along_a, own_scaled_a, 0) + rows_times(along_b, own_scaled_b, 0)
    along_other = rows_times(along_a, other_scaled_a, 0) + rows_times(along_b, other_scaled_b, 0)
    low_part, high_part = through[:half], through[half:]
    through_own = jnp.where(low_side, low_part, high_part)
    through_other = jnp.where(low_side, high_part, low_part)
    finish = lambda through, along, gain: gain * through - along / (gain * full)
    grad = finish(through_own, along_own, gain) + cross(finish(through_other, along_other, vectors_other[1]))
    grad = grad + jnp.sum(target.astype(F32) * sign[:, None], axis=0)
    bits = [1 << bit for bit in range(1, top)]
    for group in (bits[:2], bits[2:4], *([bit] for bit in bits[4:])):
        masks = [sum(bit for k, bit in enumerate(group) if n >> k & 1) for n in range(1, 1 << len(group))]
        grad = sum([permute(grad, lambda i, mask=mask: mask) for mask in masks], grad)
    return mixed, grad


def general_body(hidden, steering, norm_gain, target, routes, gate_probs, contrast, gate_weight, up_weight, down_weight):
    _, width = hidden.shape
    groups, parts = lax.axis_size("dp"), lax.axis_size("mp")
    local_experts = gate_weight.shape[0]
    full = width * parts
    here, side = lax.axis_index("dp"), lax.axis_index("mp")

    def gather(value):
        return lax.all_gather(lax.all_gather(value, "mp", axis=1, tiled=True), "dp", axis=0, tiled=True)

    sign = (2 * contrast - 1).astype(F32)
    weights = token_weights(routes, gate_probs, local_experts * groups)
    facts = lax.all_gather(jnp.concatenate([weights, sign[:, None]], axis=1), "dp", axis=0, tiled=True)
    steer_row = lax.all_gather(steering, "mp", axis=0, tiled=True)[None, :]
    gain_row = lax.all_gather(norm_gain.astype(F32), "mp", axis=0, tiled=True)[None, :]
    stream = gather(hidden).astype(F32) + steer_row
    inverse = lax.rsqrt(jnp.mean(stream * stream, axis=1, keepdims=True) + EPSILON)
    normed = (stream * inverse * gain_row).astype(BF16)
    all_target = gather(target)
    out, through, share = 0.0, 0.0, 0.0
    for k in range(local_experts):
        weight = lax.dynamic_index_in_dim(facts, here * local_experts + k, axis=1)
        gate_pre, up_pre = forward(normed, gate_weight[k], up_weight[k])
        out = out + outputs(gate_pre, up_pre, weight, down_weight[k]).astype(F32)
        vg, vu, part = pullback(gate_pre, up_pre, weight * facts[:, -1:], inverse, all_target, down_weight[k])
        through = through + rows_times(vg, gate_weight[k], 1) + rows_times(vu, up_weight[k], 1)
        share = share + part
    out = lax.psum_scatter(out.astype(BF16), "mp", scatter_dimension=1, tiled=True)
    out_tok = lax.psum_scatter(out, "dp", scatter_dimension=0, tiled=True).astype(F32)
    mixed = (hidden.astype(F32) + steering[None, :] + out_tok).astype(BF16)
    along = rows_times(share * inverse[:, 0], normed, 0)
    partial = gain_row[0] * through - along / (gain_row[0] * full)
    own = jnp.sum(target.astype(F32) * sign[:, None], axis=0)
    grad = lax.psum(partial, "mp")
    grad = lax.dynamic_slice_in_dim(grad, side * width, width) + own
    return mixed, lax.psum(grad, "dp")


def solution(mesh):
    groups, parts = mesh.shape["dp"], mesh.shape["mp"]
    fast = parts == 2 and 8 <= groups <= 32 and groups & (groups - 1) == 0

    def body(*args):
        if fast and args[7].shape[0] == 1:
            return fast_body(*args)
        return general_body(*args)

    placed = (
        P("dp", "mp"),
        P("mp"),
        P("mp"),
        P("dp", "mp"),
        P("dp", None),
        P("dp", None),
        P("dp"),
        P("dp", None, "mp"),
        P("dp", None, "mp"),
        P("dp", "mp", None),
    )
    return jax.shard_map(
        body, mesh=mesh, in_specs=placed, out_specs=(P("dp", "mp"), P("mp")), check_vma=False
    )
```

```python
import jax
import jax.numpy as jnp
from jax import lax
from jax.experimental import pallas as pl
from jax.experimental.pallas import tpu as pltpu
from jax.sharding import PartitionSpec as P

EPSILON = 1e-06
BF16 = jnp.bfloat16
F32 = jnp.float32
BOTH = ("dp", "mp")


def thirds(values):
    high = lax.reduce_precision(values, 8, 7)
    rest = values - high
    middle = lax.reduce_precision(rest, 8, 7)
    low = rest - middle
    return high.astype(BF16), middle.astype(BF16), low.astype(BF16)


def rows_times(values, matrix, contracted):
    rows = lax.optimization_barrier(jnp.stack(thirds(values)))
    return jnp.sum(
        lax.dot_general(rows, matrix, (((1,), (contracted,)), ((), ())), preferred_element_type=F32),
        axis=0,
    )


def forward(normed, gate_mat, up_mat):
    gate_pre = jnp.dot(normed, gate_mat, preferred_element_type=F32)
    up_pre = jnp.dot(normed, up_mat, preferred_element_type=F32)
    return lax.optimization_barrier((gate_pre, up_pre))


def outputs(gate_pre, up_pre, weight, down_mat):
    activated = lax.optimization_barrier((gate_pre * jax.nn.sigmoid(gate_pre) * up_pre).astype(BF16))
    out = jnp.dot(activated, down_mat, preferred_element_type=F32)
    return (out * weight).astype(BF16)


def pullback(gate_pre, up_pre, scale, inverse, rows, down_mat):
    back = lax.dot_general(rows, down_mat, (((1,), (1,)), ((), ())), preferred_element_type=F32)
    back = lax.optimization_barrier(back) * scale
    sigma = jax.nn.sigmoid(gate_pre)
    grad_gate = back * up_pre * sigma * (1.0 + gate_pre * (1.0 - sigma))
    grad_up = back * gate_pre * sigma
    share = jnp.sum(grad_gate * gate_pre + grad_up * up_pre, axis=1)
    return jnp.sum(grad_gate * inverse, axis=0), jnp.sum(grad_up * inverse, axis=0), share


def token_weights(routes, gate_probs, experts):
    named = routes[:, :, None] == jnp.arange(experts, dtype=jnp.int32)
    return jnp.sum(jnp.where(named, gate_probs[:, :, None], 0.0), axis=1)


def after(value, *others):
    return lax.optimization_barrier((value, *others))[0]


def tile_of(size, most):
    return max(t for t in range(128, most + 1, 128) if size % t == 0)


VMEM = pl.BlockSpec(memory_space=pltpu.VMEM)
SMEM = pl.BlockSpec(memory_space=pltpu.SMEM)
ANY = pl.BlockSpec(memory_space=pltpu.HBM)


def call(kernel, operands, specs, outs, scratch, megabytes, flops, moved):
    return pl.pallas_call(
        kernel,
        in_specs=specs,
        out_specs=[VMEM] * len(outs),
        out_shape=[jax.ShapeDtypeStruct(shape, dtype) for shape, dtype in outs],
        scratch_shapes=scratch,
        compiler_params=pltpu.CompilerParams(vmem_limit_bytes=megabytes << 20),
        cost_estimate=pl.CostEstimate(flops=flops, bytes_accessed=moved, transcendentals=0),
    )(*operands)


CHUNK = 16
WEIGHT, SIGNED, SQUARES, INVERSE = 0, 1, 2, 3


def column(array, index):
    return array[:, index : index + 1]


def facts_of(columns):
    rows = columns[0].shape[0]
    lane = lax.broadcasted_iota(jnp.int32, (rows, 128), 1)
    found = jnp.zeros((rows, 128), F32)
    for index, values in enumerate(columns):
        found = jnp.where(lane == index, values, found)
    return found


def scale_rows(blocks, steer, gain, scaled, squares):
    first, half = 0, scaled.shape[1]
    for source in blocks:
        group = next(g for g in (4, 2, 1) if source.shape[0] % (g * CHUNK) == 0)

        def chunks(number, carry, source=source, first=first, group=group):
            for k in range(group):
                at = pl.multiple_of((number * group + k) * CHUNK, CHUNK)
                stream = source[pl.ds(at, CHUNK), :half].astype(F32) + steer
                scaled[pl.ds(first + at, CHUNK), :] = (stream * gain).astype(BF16)
                square = stream * stream
                squares[pl.ds(first + at, CHUNK), :] = sum(square[:, c : c + 128] for c in range(0, half, 128))
            return carry

        lax.fori_loop(0, source.shape[0] // (group * CHUNK), chunks, 0)
        first += source.shape[0]


def fetches(source, buffer, sems, view, ahead=2):
    count, slots = sems.shape[0], buffer.shape[0]
    copies = lambda i: pltpu.make_async_copy(view(source, i), buffer.at[lax.rem(i, slots)], sems.at[i])
    for i in range(min(ahead, count)):
        copies(i).start()

    def take(i):
        copies(i).wait()

        @pl.when(i + ahead < count)
        def _():
            copies(i + ahead).start()

    return take


def split_dot(rows, matrix):
    middle = rows.shape[0] // 2
    return jnp.concatenate(
        [jnp.dot(rows[part, :], matrix, preferred_element_type=F32) for part in (slice(0, middle), slice(middle, None))], axis=0
    )


def half_fetches(gate_mat, up_mat, gate_buf, up_buf, gate_sems, up_sems, chosen):
    tile = gate_buf.shape[2]
    view = lambda source, i: source.at[chosen, :, pl.ds(i * tile, tile)]
    return fetches(gate_mat, gate_buf, gate_sems, view), fetches(up_mat, up_buf, up_sems, view)


def own_kernel(experts, which, a, b, steer, gain, gate_mat, up_mat, gate_acc, up_acc, scaled, facts, gate_buf, up_buf, gate_sems, up_sems, squares):
    gate_wait, up_wait = half_fetches(gate_mat, up_mat, gate_buf, up_buf, gate_sems, up_sems, which[0])
    half, tile = scaled.shape[1], gate_buf.shape[2]
    scale_rows((a, b), steer[which[0]], gain[which[0]], scaled, squares)
    first = 0
    for source in (a, b):
        rows = slice(first, first + source.shape[0])
        values = source[:, half:].astype(F32)
        lane = lax.broadcasted_iota(jnp.int32, values.shape, 1)
        mine = (lane == which[2]) | (lane == which[2] + experts) | (lane == which[2] + 2 * experts)
        weight = jnp.sum(jnp.where(mine, values, 0.0), axis=1, keepdims=True)
        sign = jnp.sum(jnp.where(lane == 3 * experts, values, 0.0), axis=1, keepdims=True)
        facts[rows, :] = facts_of([weight, weight * sign, jnp.sum(squares[rows, :], axis=1, keepdims=True)])
        first += source.shape[0]

    def step(i, carry):
        at = pl.ds(pl.multiple_of(i * tile, tile), tile)
        gate_wait(i)
        gate_acc[:, at] = split_dot(scaled, gate_buf[i])
        up_wait(i)
        up_acc[:, at] = split_dot(scaled, up_buf[i])
        return carry

    lax.fori_loop(0, gate_buf.shape[0], step, 0)


def other_kernel(which, a, b, c, d, steer, gain, gate_mat, up_mat, *refs):
    states, outs, scratch = (refs[0:3], refs[3:6]), (refs[6:11], refs[11:16]), refs[16:]
    gate_buf, up_buf, gate_sems, up_sems, squares = scratch
    gate_wait, up_wait = half_fetches(gate_mat, up_mat, gate_buf, up_buf, gate_sems, up_sems, which[1])
    half, tile = a.shape[1] - 128, gate_buf.shape[2]
    for blocks, state, out in zip(((a, b), (c, d)), states, outs):
        scaled, found, old = out[3], out[4], state[2][...]
        scale_rows(blocks, steer[which[1]], gain[which[1]], scaled, squares)
        total = column(old, SQUARES) + jnp.sum(squares[...], axis=1, keepdims=True)
        found[...] = facts_of([column(old, WEIGHT), column(old, SIGNED), total, lax.rsqrt(total / (2 * half) + EPSILON)])

    def step(i, carry):
        at = pl.ds(pl.multiple_of(i * tile, tile), tile)
        gate_wait(i)
        for (gate_acc, _, _), (gate_pre, _, _, scaled, found) in zip(states, outs):
            gate = gate_acc[:, at] + jnp.dot(scaled[...], gate_buf[i], preferred_element_type=F32)
            gate_pre[:, at] = gate * column(found[...], INVERSE)
        up_wait(i)
        for (_, up_acc, _), (gate_pre, up_pre, activated, scaled, found) in zip(states, outs):
            up = up_acc[:, at] + jnp.dot(scaled[...], up_buf[i], preferred_element_type=F32)
            up, gate = up * column(found[...], INVERSE), gate_pre[:, at]
            up_pre[:, at] = up
            activated[:, at] = (gate * jax.nn.sigmoid(gate) * up).astype(BF16)
        return carry

    lax.fori_loop(0, gate_buf.shape[0], step, 0)


def half_products(which, blocks, steer, gain, gate_mat, up_mat, states=()):
    half, units = gate_mat.shape[1:]
    rows, tile = 2 * blocks[0].shape[0], tile_of(units, 256)
    unit, wide, facts = ((rows, units), F32), ((rows, half), BF16), ((rows, 128), F32)
    buffer, sems = pltpu.VMEM((units // tile, half, tile), BF16), pltpu.SemaphoreType.DMA((units // tile,))
    operands = [which, *blocks, steer, gain, gate_mat, up_mat, *(v for state in states for v in state)]
    specs = [SMEM] + [VMEM] * (len(blocks) + 2) + [ANY] * 2 + [VMEM] * (3 * len(states))
    if states:
        kernel = other_kernel
        outs = [unit, unit, ((rows, units), BF16), wide, facts] * 2
    else:
        experts = lax.axis_size("dp")
        kernel = lambda *refs: own_kernel(experts, *refs)
        outs = [unit, unit, wide, facts]
    return call(
        kernel,
        operands,
        specs,
        outs,
        [buffer, buffer, sems, sems, pltpu.VMEM((rows, 128), F32)],
        35,
        2 * len(blocks) * rows * half * units,
        4 * half * units,
    )


def out_kernel(chosen, which, act_a, act_b, facts_a, facts_b, down_mat, near, far, buf, sems):
    tiles, _, tile = buf.shape
    height = act_a.shape[0] // 2
    start = which[chosen] * (tile * tiles)
    take = fetches(down_mat, buf, sems, lambda source, i: source.at[:, pl.ds(pl.multiple_of(start + i * tile, tile), tile)], 3)

    def step(i, carry):
        at = pl.ds(pl.multiple_of(i * tile, tile), tile)
        take(i)
        for first, activated, facts in ((0, act_a, facts_a), (height, act_b, facts_b)):
            out = jnp.dot(activated[...], buf[i], preferred_element_type=F32) * column(facts[...], WEIGHT)
            near[first : first + height, at] = out[:height].astype(BF16)
            far[first : first + height, at] = out[height:].astype(BF16)
        return carry

    lax.fori_loop(0, tiles, step, 0)


def expert_out(chosen, which, acts, facts, down_mat):
    rows, units = acts[0].shape
    half = down_mat.shape[1] // 2
    tile = tile_of(half, 512)
    out = ((rows, half), BF16)
    return call(
        lambda *refs: out_kernel(chosen, *refs),
        (which, *acts, *facts, down_mat),
        [SMEM] + [VMEM] * 4 + [ANY],
        [out, out],
        [pltpu.VMEM((half // tile, units, tile), BF16), pltpu.SemaphoreType.DMA((half // tile,))],
        37,
        4 * rows * half * units,
        2 * half * units,
    )


def back_kernel(which, near_own, far_own, near_other, far_other, gate_a, gate_b, up_a, up_b, facts_a, facts_b, down_mat, gate_sum, up_sum, share_a, share_b, own_buf, other_buf, own_sems, other_sems):
    tile, half = own_buf.shape[1:]
    view = lambda h: lambda source, i: source.at[pl.ds(i * tile, tile), pl.ds(pl.multiple_of(which[h] * half, half), half)]
    own_take = fetches(down_mat, own_buf, own_sems, view(0))
    other_take = fetches(down_mat, other_buf, other_sems, view(1))
    dims = (((1,), (1,)), ((), ()))
    share_a[...] = jnp.zeros_like(share_a)
    share_b[...] = jnp.zeros_like(share_b)
    height = near_own.shape[0] // 2
    groups = ((gate_a, up_a, facts_a, share_a), (gate_b, up_b, facts_b, share_b))

    def step(i, carry):
        at = pl.ds(pl.multiple_of(i * tile, tile), tile)
        own_take(i)
        other_take(i)
        gate_total, up_total = 0.0, 0.0
        for first, own, other in ((0, near_own, near_other), (height, far_own, far_other)):
            product = lax.dot_general(own[...], own_buf[i], dims, preferred_element_type=F32)
            product += lax.dot_general(other[...], other_buf[i], dims, preferred_element_type=F32)
            rows = slice(first, first + height)
            for number, (gate_pre, up_pre, facts, share) in enumerate(groups):
                known = facts[rows, :]
                back = product[number * height : (number + 1) * height] * column(known, SIGNED)
                gate, up = gate_pre[rows, at], up_pre[rows, at]
                sigma = jax.nn.sigmoid(gate)
                grad_gate = back * up * sigma * (1.0 + gate * (1.0 - sigma))
                grad_up = back * gate * sigma
                inverse = column(known, INVERSE)
                gate_total += jnp.sum(grad_gate * inverse, axis=0, keepdims=True)
                up_total += jnp.sum(grad_up * inverse, axis=0, keepdims=True)
                part = grad_gate * gate + grad_up * up
                share[rows, :] += sum(part[:, c : c + 128] for c in range(0, tile, 128))
        gate_sum[:, at] = gate_total
        up_sum[:, at] = up_total
        return carry

    lax.fori_loop(0, own_buf.shape[0], step, 0)


def expert_back(which, rows_of, down_mat, gate_pre, up_pre, facts):
    half = rows_of[0].shape[1]
    rows, units = gate_pre[0].shape
    tile = tile_of(units, 256)
    buffer, sems = pltpu.VMEM((units // tile, tile, half), BF16), pltpu.SemaphoreType.DMA((units // tile,))
    return call(
        back_kernel,
        (which, *rows_of, *gate_pre, *up_pre, *facts, down_mat),
        [SMEM] + [VMEM] * 10 + [ANY],
        [((1, units), F32), ((1, units), F32), ((rows, 128), F32), ((rows, 128), F32)],
        [buffer, buffer, sems, sems],
        37,
        8 * rows * half * units,
        4 * half * units,
    )


def through_kernel(gate_sum, up_sum, gate_mat, up_mat, out, gate_buf, up_buf, gate_sems, up_sems):
    slots, tile, units = gate_buf.shape
    view = lambda source, i: source.at[pl.ds(i * tile, tile), :]
    gate_wait = fetches(gate_mat, gate_buf, gate_sems, view)
    up_wait = fetches(up_mat, up_buf, up_sems, view)
    chunk = 128

    def step(i, carry):
        gate_wait(i)
        up_wait(i)
        slot = lax.rem(i, slots)
        for r in range(tile // chunk):
            at = pl.ds(r * chunk, chunk)
            total = jnp.zeros((chunk, 128), F32)
            for c in range(0, units, 128):
                lanes = slice(c, c + 128)
                total += gate_buf[slot, at, lanes].astype(F32) * gate_sum[:, lanes]
                total += up_buf[slot, at, lanes].astype(F32) * up_sum[:, lanes]
            to = pl.ds(pl.multiple_of(i * tile + r * chunk, chunk), chunk)
            out[:, to] = jnp.sum(total.T, axis=0, keepdims=True)
        return carry

    lax.fori_loop(0, gate_sems.shape[0], step, 0)


def through_weights(gate_sum, up_sum, gate_mat, up_mat):
    full, units = gate_mat.shape
    tile = tile_of(full, 896)
    buffer, sems = pltpu.VMEM((4, tile, units), BF16), pltpu.SemaphoreType.DMA((full // tile,))
    return call(
        through_kernel,
        (gate_sum, up_sum, gate_mat, up_mat),
        [VMEM, VMEM, ANY, ANY],
        [((1, full), F32)],
        [buffer, buffer, sems, sems],
        40,
        512 * full * units,
        4 * full * units,
    )[0]


def fast_body(hidden, steering, norm_gain, target, routes, gate_probs, contrast, gate_weight, up_weight, down_weight):
    tokens, half = hidden.shape
    devices = 2 * lax.axis_size("dp")
    experts = lax.axis_size("dp")
    full = 2 * half
    gate_mat, up_mat, down_mat = gate_weight[0], up_weight[0], down_weight[0]
    gate_halves = gate_mat.reshape(2, half, gate_mat.shape[1])
    up_halves = up_mat.reshape(2, half, up_mat.shape[1])
    here, side = lax.axis_index("dp"), lax.axis_index("mp")
    even = here % 2 == 0
    low_side = side == 0
    which = jnp.stack([side, 1 - side, here]).astype(jnp.int32)
    top = devices.bit_length() - 1
    falling = [1 << b for b in range(top - 1, 2, -1)]
    orders = (falling + [1 << 2, 1], [1 << 2] + falling[:-1] + [1, falling[-1]])
    steps = len(falling) + 2
    last, third = steps - 1, steps - 2

    def permute(value, mask):
        return lax.ppermute(value, BOTH, [(i, i ^ mask(i)) for i in range(devices)])

    def hop(value, step):
        return permute(value, lambda i: orders[(i >> 1) & 1][step])

    def swap(value):
        return permute(value, lambda i: 2)

    def cross(value):
        return permute(value, lambda i: 1)

    def spread(value, gates=None):
        hold = (lambda v, g: after(v, *gates[g])) if gates else (lambda v, g: v)
        held = hold(value, 0)
        for step in range(steps - 3):
            held = jnp.concatenate([held, hop(held, step)], axis=0)
        p0 = hold(held, 1)
        p1 = hop(p0, steps - 3)
        p4 = hop(p0, last)
        p2 = hop(p0, third)
        p1, p2 = hold(p1, 2), hold(p2, 2)
        p3 = hop(p1, third)
        p5 = hop(p1, last)
        p6 = hop(p2, last)
        p7 = hop(hold(p3, 3), last)
        return p0, p1, p2, p3, p4, p5, p6, p7

    def quarters(p):
        own_b = jnp.where(even, p[2], p[4]), jnp.where(even, p[3], p[5])
        other_a = jnp.where(even, p[4], p[2]), jnp.where(even, p[5], p[3])
        return (p[0], p[1]), own_b, other_a, (p[6], p[7])

    gain = norm_gain.astype(F32)
    sign = (2 * contrast - 1).astype(F32)
    weights = token_weights(routes, gate_probs, experts)
    meta = jnp.concatenate([*thirds(weights), sign.astype(BF16)[:, None]], axis=1)
    meta = jnp.pad(meta, ((0, 0), (0, 128 - meta.shape[1])))
    vectors = jnp.stack([steering, gain])
    vectors_other = cross(vectors)
    steer_halves = jnp.where(low_side, jnp.stack([vectors[0], vectors_other[0]]), jnp.stack([vectors_other[0], vectors[0]]))
    gain_halves = jnp.where(low_side, jnp.stack([vectors[1], vectors_other[1]]), jnp.stack([vectors_other[1], vectors[1]]))
    steer_halves, gain_halves = steer_halves[:, None, :], gain_halves[:, None, :]

    pieces = spread(jnp.concatenate([hidden, meta], axis=1))
    own_a, own_b, other_a, other_b = (jnp.concatenate(pair, axis=0) for pair in quarters(pieces))
    shared = (steer_halves, gain_halves, gate_halves, up_halves)
    state_a = half_products(which, (own_a, swap(own_a)), *shared)
    far_other_a = swap(other_a)
    state_b = half_products(which, (own_b, swap(own_b)), *shared)
    split = lambda state: ((state[0], state[1], state[3]), state[2])
    (state_a, own_scaled_a), (state_b, own_scaled_b) = split(state_a), split(state_b)
    blocks = other_a, far_other_a, other_b, swap(other_b)
    done = half_products(which, blocks, *shared, (state_a, state_b))
    (gate_a, up_a, act_a, other_scaled_a, facts_a), (gate_b, up_b, act_b, other_scaled_b, facts_b) = done[:5], done[5:]
    facts = facts_a, facts_b
    near_other, far_other = expert_out(1, which, (act_a, act_b), facts, down_mat)
    here_other = swap(far_other)
    near_own, far_own = expert_out(0, which, (act_a, after(act_b, near_other)), facts, down_mat)
    here_own = swap(far_own)

    gates = (pieces[3], pieces[5]), (pieces[6], pieces[7]), (act_b,), (near_other,)
    targets = spread(target, gates)

    def add(*addends):
        return sum(a.astype(F32) for a in addends).astype(BF16)

    rows = near_own.shape[0] // 4
    sum_own, sum_other = (near_own, here_own), (near_other, here_other)
    piece = lambda pair, i: add(*(v[i * rows : (i + 1) * rows] for v in pair))
    a7, a6 = piece(sum_other, 3), piece(sum_other, 2)
    sum_own = near_own, after(here_own, a7, a6)
    a5 = jnp.where(even, piece(sum_other, 1), piece(sum_own, 3))
    a4 = jnp.where(even, piece(sum_other, 0), piece(sum_own, 2))
    a3 = jnp.where(even, piece(sum_own, 3), piece(sum_other, 1))
    a2 = jnp.where(even, piece(sum_own, 2), piece(sum_other, 0))
    a1, a0 = piece(sum_own, 1), piece(sum_own, 0)
    b3 = hop(a7, last)
    b2 = hop(a6, last)
    b1 = hop(a5, last)
    b0 = hop(a4, last)
    third1 = add(a3, b3)
    c1 = hop(third1, third)

    own_a, own_b, other_a, other_b = quarters([after(v, a7, a6, a5, a4) for v in targets])
    target_own = jnp.concatenate(own_a + own_b, axis=0)
    target_other = jnp.concatenate(other_a + other_b, axis=0)
    far = swap(target_own), swap(target_other)
    rows_of = after(target_own, third1), far[0], target_other, far[1]
    gate_sum, up_sum, share_a, share_b = expert_back(which, rows_of, down_mat, (gate_a, gate_b), (up_a, up_b), facts)
    third0 = add(after(a2, gate_sum), b2)
    c0 = hop(third0, third)
    early = add(a1, b1, c1)
    d0 = hop(early, steps - 3)
    addends = [a0, b0, c0, d0]
    for step in range(steps - 4, -1, -1):
        rows //= 2
        addends.append(hop(add(*(a[rows : 2 * rows] for a in addends)), step))
    out_tok = sum(a[:tokens].astype(F32) for a in addends)
    mixed = (hidden.astype(F32) + steering[None, :] + out_tok).astype(BF16)
    through = through_weights(after(gate_sum, third0, early), up_sum, gate_mat, up_mat)[0]
    weigh = lambda share, facts: jnp.sum(after(share, early), axis=1) * facts[:, INVERSE] * facts[:, INVERSE]
    along_a, along_b = weigh(share_a, facts_a), weigh(share_b, facts_b)
    along_own = rows_times(along_a, own_scaled_a, 0) + rows_times(along_b, own_scaled_b, 0)
    along_other = rows_times(along_a, other_scaled_a, 0) + rows_times(along_b, other_scaled_b, 0)
    low_part, high_part = through[:half], through[half:]
    through_own = jnp.where(low_side, low_part, high_part)
    through_other = jnp.where(low_side, high_part, low_part)
    finish = lambda through, along, gain: gain * through - along / (gain * full)
    grad = finish(through_own, along_own, gain) + cross(finish(through_other, along_other, vectors_other[1]))
    grad = grad + jnp.sum(target.astype(F32) * sign[:, None], axis=0)
    bits = [1 << bit for bit in range(1, top)]
    for group in (bits[:2], bits[2:4], *([bit] for bit in bits[4:])):
        masks = [sum(bit for k, bit in enumerate(group) if n >> k & 1) for n in range(1, 1 << len(group))]
        grad = sum([permute(grad, lambda i, mask=mask: mask) for mask in masks], grad)
    return mixed, grad


def general_body(hidden, steering, norm_gain, target, routes, gate_probs, contrast, gate_weight, up_weight, down_weight):
    _, width = hidden.shape
    groups, parts = lax.axis_size("dp"), lax.axis_size("mp")
    local_experts = gate_weight.shape[0]
    full = width * parts
    here, side = lax.axis_index("dp"), lax.axis_index("mp")

    def gather(value):
        return lax.all_gather(lax.all_gather(value, "mp", axis=1, tiled=True), "dp", axis=0, tiled=True)

    sign = (2 * contrast - 1).astype(F32)
    weights = token_weights(routes, gate_probs, local_experts * groups)
    facts = lax.all_gather(jnp.concatenate([weights, sign[:, None]], axis=1), "dp", axis=0, tiled=True)
    steer_row = lax.all_gather(steering, "mp", axis=0, tiled=True)[None, :]
    gain_row = lax.all_gather(norm_gain.astype(F32), "mp", axis=0, tiled=True)[None, :]
    stream = gather(hidden).astype(F32) + steer_row
    inverse = lax.rsqrt(jnp.mean(stream * stream, axis=1, keepdims=True) + EPSILON)
    normed = (stream * inverse * gain_row).astype(BF16)
    all_target = gather(target)
    out, through, share = 0.0, 0.0, 0.0
    for k in range(local_experts):
        weight = lax.dynamic_index_in_dim(facts, here * local_experts + k, axis=1)
        gate_pre, up_pre = forward(normed, gate_weight[k], up_weight[k])
        out = out + outputs(gate_pre, up_pre, weight, down_weight[k]).astype(F32)
        vg, vu, part = pullback(gate_pre, up_pre, weight * facts[:, -1:], inverse, all_target, down_weight[k])
        through = through + rows_times(vg, gate_weight[k], 1) + rows_times(vu, up_weight[k], 1)
        share = share + part
    out = lax.psum_scatter(out.astype(BF16), "mp", scatter_dimension=1, tiled=True)
    out_tok = lax.psum_scatter(out, "dp", scatter_dimension=0, tiled=True).astype(F32)
    mixed = (hidden.astype(F32) + steering[None, :] + out_tok).astype(BF16)
    along = rows_times(share * inverse[:, 0], normed, 0)
    partial = gain_row[0] * through - along / (gain_row[0] * full)
    own = jnp.sum(target.astype(F32) * sign[:, None], axis=0)
    grad = lax.psum(partial, "mp")
    grad = lax.dynamic_slice_in_dim(grad, side * width, width) + own
    return mixed, lax.psum(grad, "dp")


def solution(mesh):
    groups, parts = mesh.shape["dp"], mesh.shape["mp"]
    fast = parts == 2 and 8 <= groups <= 32 and groups & (groups - 1) == 0

    def body(*args):
        if fast and args[7].shape[0] == 1:
            return fast_body(*args)
        return general_body(*args)

    placed = (
        P("dp", "mp"),
        P("mp"),
        P("mp"),
        P("dp", "mp"),
        P("dp", None),
        P("dp", None),
        P("dp"),
        P("dp", None, "mp"),
        P("dp", None, "mp"),
        P("dp", "mp", None),
    )
    return jax.shard_map(
        body, mesh=mesh, in_specs=placed, out_specs=(P("dp", "mp"), P("mp")), check_vma=False
    )
```
